32 devices in a mesh: gx: 8 (over y, x, core), gy: 4 (over z).
Axes of the slice: x: 2, y: 2, z: 4, core: 2. Of those that a mesh axis runs over, the one named last changes fastest.
Arguments:
- coefficients: float32 [2, 2048, 512], P(None, 'gx', 'gy'), may hold values from -0.125 to 0.125
- spacing: float32 [31], replicated, may hold values from 0.6 to 1.5
Outputs:
- zcoord: float32 [32, 4096, 512], P(None, 'gx', 'gy')
- slopes: float32 [2, 32, 4096, 512], P(None, None, 'gx', 'gy')
- jacobian: float32 [32, 4096, 512], P(None, 'gx', 'gy')
- quality: float32 [32, 4096, 512], P(None, 'gx', 'gy')
The draws below stay inside these ranges and needn't reach their ends.
All inputs are finite; a program needn't handle non-finite values.
Results may differ from the reference program's by a relative error of at most 0.0003.
Values sent between devices are 32-bit elements; how exact they have to be, the bound alone decides.
A program may use at most 128 MiB of HBM per device.

```python
import math
import jax
import jax.numpy as jnp
from jax import lax

NX = 4096
MODES = 2048
NY = 512
GAPS = 31


def shard_levels(own_key, shape, shards, least, high):
    factor_of, own = 1.0, jax.random.fold_in(own_key, 6)
    for axis_at, shards_of in shards:
        steps = jnp.exp(jax.random.uniform(jax.random.fold_in(own, axis_at), (shards_of,), jnp.float32, least / len(shards), high / len(shards)))
        factor_of = factor_of * jnp.repeat(steps, shape[axis_at] // shards_of).reshape([-1 if axis == axis_at else 1 for axis in range(len(shape))])
    return factor_of


def bell_draw(stream_key, dims, scale, reach, split=(), held_as=jnp.bfloat16):
    drawn = scale * jax.random.normal(stream_key, dims, jnp.float32)
    if split:
        drawn = drawn * shard_levels(stream_key, dims, split, -0.22, 0.18)
    return jnp.clip(drawn, -reach, reach).astype(held_as)


def setup_inputs(seed: int = 0) -> dict:
    streams_of = jax.random.split(jax.random.key(seed), 3)
    coefficients = bell_draw(streams_of[0], (2, MODES, NY), MODES ** -0.5, 0.125, ((1, 8), (2, 4)), jnp.float32)
    spacing = jnp.clip(jnp.exp(jax.random.uniform(streams_of[1], (GAPS,), jnp.float32, math.log(0.6), math.log(1.5))), 0.6, 1.5)
    return {"coefficients": coefficients, "spacing": spacing}


BOUNDARY = ((-24.0 / 17.0, 59.0 / 34.0, -4.0 / 17.0, -3.0 / 34.0, 0.0, 0.0), (-0.5, 0.0, 0.5, 0.0, 0.0, 0.0), (4.0 / 43.0, -59.0 / 86.0, 0.0, 59.0 / 86.0, -4.0 / 43.0, 0.0), (3.0 / 98.0, 0.0, -59.0 / 98.0, 0.0, 32.0 / 49.0, -4.0 / 49.0))
TOPO_SCALE = 0.1


def vertical(field):
    levels = field.shape[0]
    top_rows = []
    bottom_rows = []
    for row_id in range(4):
        upper = None
        lower = None
        for level_id, factor in enumerate(BOUNDARY[row_id]):
            if factor != 0.0:
                term_up = factor * field[level_id]
                term_down = -factor * field[levels - 1 - level_id]
                upper = term_up if upper is None else upper + term_up
                lower = term_down if lower is None else lower + term_down
        top_rows.append(upper)
        bottom_rows.append(lower)
    inner = (8.0 * (field[5:levels - 3] - field[3:levels - 5]) - (field[6:levels - 2] - field[2:levels - 6])) / 12.0
    return jnp.concatenate([jnp.stack(top_rows), inner, jnp.stack(bottom_rows[::-1])], axis=0)


def stretching(spacing):
    summed = jnp.sum(spacing)
    return jnp.concatenate([jnp.zeros((1,), spacing.dtype), jnp.cumsum(spacing)]) / summed


def column_depth(surface, stretch):
    levels = stretch.shape[0]
    return (levels - 1.0) * (surface[None] + (1.0 - surface[None]) * stretch[:, None, None])


def across(field, axis_id):
    plus_one = jnp.roll(field, -1, axis_id)
    minus_one = jnp.roll(field, 1, axis_id)
    plus_two = jnp.roll(field, -2, axis_id)
    minus_two = jnp.roll(field, 2, axis_id)
    return (8.0 * (plus_one - minus_one) - (plus_two - minus_two)) / 12.0


def reference(coefficients, spacing):
    mode_ids = jnp.arange(MODES, dtype=jnp.int32)
    x_cells = jnp.arange(NX, dtype=jnp.int32)
    phase = ((mode_ids[:, None] * x_cells[None, :]) % NX).astype(jnp.float32) * (2.0 * math.pi / NX)
    cosine = jnp.cos(phase)
    sine = jnp.sin(phase)
    surface_raw = jnp.dot(cosine.T, coefficients[0], precision=lax.Precision.HIGHEST, preferred_element_type=jnp.float32)
    surface_raw = surface_raw + jnp.dot(sine.T, coefficients[1], precision=lax.Precision.HIGHEST, preferred_element_type=jnp.float32)
    surface = TOPO_SCALE * jnp.tanh(surface_raw * 0.25)
    stretch = stretching(spacing)
    zcoord = column_depth(surface, stretch)
    slopes = jnp.stack([across(zcoord, 1), across(zcoord, 2)])
    jacobian = vertical(zcoord)
    lowest = jnp.min(jacobian)
    quality = jacobian / lowest
    return zcoord, slopes, jacobian, quality
```

```python
import functools
import math

import jax
import jax.numpy as jnp
import numpy as np
from jax import lax
from jax.experimental import pallas as pl
from jax.experimental.pallas import tpu as pltpu
from jax.sharding import PartitionSpec as P

NX = 4096


BOUNDARY = (
    (-24.0 / 17.0, 59.0 / 34.0, -4.0 / 17.0, -3.0 / 34.0, 0.0, 0.0),
    (-0.5, 0.0, 0.5, 0.0, 0.0, 0.0),
    (4.0 / 43.0, -59.0 / 86.0, 0.0, 59.0 / 86.0, -4.0 / 43.0, 0.0),
    (3.0 / 98.0, 0.0, -59.0 / 98.0, 0.0, 32.0 / 49.0, -4.0 / 49.0),
)
TOPO_SCALE = 0.1


def extended(cells, sides, width):
    for axis, dim in sides:
        count = lax.axis_size(axis)
        head = lax.slice_in_dim(cells, 0, width, axis=dim)
        tail = lax.slice_in_dim(cells, cells.shape[dim] - width, cells.shape[dim], axis=dim)
        cells = jnp.concatenate(
            [
                lax.ppermute(tail, axis, [(i, (i + 1) % count) for i in range(count)]),
                cells,
                lax.ppermute(head, axis, [((i + 1) % count, i) for i in range(count)]),
            ],
            axis=dim,
        )
    return cells


def vertical(field):
    levels = field.shape[0]
    top_rows = []
    bottom_rows = []
    for row_id in range(4):
        upper = None
        lower = None
        for level_id, factor in enumerate(BOUNDARY[row_id]):
            if factor != 0.0:
                term_up = factor * field[level_id]
                term_down = -factor * field[levels - 1 - level_id]
                upper = term_up if upper is None else upper + term_up
                lower = term_down if lower is None else lower + term_down
        top_rows.append(upper)
        bottom_rows.append(lower)
    inner = (
        8.0 * (field[5 : levels - 3] - field[3 : levels - 5])
        - (field[6 : levels - 2] - field[2 : levels - 6])
    ) / 12.0
    return jnp.concatenate([jnp.stack(top_rows), inner, jnp.stack(bottom_rows[::-1])], axis=0)


def stretching(spacing):
    summed = jnp.sum(spacing)
    return jnp.concatenate([jnp.zeros((1,), spacing.dtype), jnp.cumsum(spacing)]) / summed


def column_depth(surface, stretch):
    levels = stretch.shape[0]
    return (levels - 1.0) * (surface[None] + (1.0 - surface[None]) * stretch[:, None, None])


def basis(count, x_cells):
    mode_ids = jnp.arange(count, dtype=jnp.int32)
    phase = (mode_ids[:, None] * x_cells[None, :] % NX).astype(jnp.float32) * (2.0 * math.pi / NX)
    return (jnp.cos(phase), jnp.sin(phase))


def project(cosine, sine, portion):
    first = jnp.dot(
        cosine.T, portion[0], precision=lax.Precision.HIGHEST, preferred_element_type=jnp.float32
    )
    return first + jnp.dot(
        sine.T, portion[1], precision=lax.Precision.HIGHEST, preferred_element_type=jnp.float32
    )


LANES = 128
RADIX = 16
TILE = 8
MESH = pl.DeviceIdType.MESH


def level_weights(gaps):
    levels = gaps + 1
    summed = np.tril(np.ones((levels, gaps)), -1)
    deriv = np.zeros((levels, levels))
    for row in range(levels):
        if row < 4:
            deriv[row, :6] = BOUNDARY[row]
        elif row >= levels - 4:
            deriv[row, ::-1][:6] = -np.array(BOUNDARY[levels - 1 - row])
        else:
            deriv[row, row - 2 : row + 3] = np.array([1.0, -8.0, 0.0, 8.0, -1.0]) / 12.0
    return np.stack([summed, deriv @ summed]).astype(np.float32)


def transform_tables(modes, groups):
    part = NX // RADIX
    own = part // groups
    block = own + TILE
    rows = []
    for dest in range(groups):
        first = dest * own
        rows += list(range(first, first + own)) + [first - 1, first + own] * (TILE // 2)
    angle = 2.0 * np.pi / part * ((np.array(rows)[:, None] * np.arange(part)[None]) % part)
    full = np.concatenate([np.cos(angle), np.sin(angle)], axis=1).astype(np.float32)
    turn = 2.0 * np.pi / NX * (np.arange(RADIX)[:, None] * np.arange(part)[None])
    twiddle = np.concatenate([np.cos(turn), np.sin(turn)], axis=1).astype(np.float32)
    return full, twiddle, block


def rotate(value, angle):
    re, im = value
    cos, sin = math.cos(angle), math.sin(angle)
    if abs(sin) < 1e-12:
        return (re, im) if cos > 0 else (-re, -im)
    if abs(cos) < 1e-12:
        return (im, -re) if sin > 0 else (-im, re)
    if abs(abs(cos) - abs(sin)) < 1e-12:
        unit = math.sqrt(0.5)
        a, b = math.copysign(1.0, cos), math.copysign(1.0, sin)
        one = re * unit if a > 0 else re * -unit
        two = im * unit if a > 0 else im * -unit
        if a == b:
            return one + two, two - one
        return one - two, two + one
    return re * cos + im * sin, im * cos - re * sin


def fourier(values):
    count = len(values)
    if count == 1:
        return values
    even, odd = fourier(values[0::2]), fourier(values[1::2])
    out = [None] * count
    for i in range(count // 2):
        re, im = rotate(odd[i], 2.0 * math.pi * i / count)
        out[i] = (even[i][0] + re, even[i][1] + im)
        out[i + count // 2] = (even[i][0] - re, even[i][1] - im)
    return out


def split(value):
    high = value.astype(jnp.bfloat16)
    return high, (value - high.astype(jnp.float32)).astype(jnp.bfloat16)


def butterfly(values, bit, lane):
    shift = bit * TILE
    upper = (lane // TILE) & bit != 0
    for i in sorted(values):
        if not i & bit and i | bit in values:
            low, high = values[i], values[i | bit]
            values[i] = jnp.where(upper, pltpu.roll(high, shift, 1), low)
            values[i | bit] = jnp.where(upper, high, pltpu.roll(low, LANES - shift, 1))
    return values


def blocks_of(chunk, groups):
    return [2 * j + (chunk + j // (groups // 2)) % 2 for j in range(groups)]


def arrived(view, sem):
    pltpu.make_async_copy(view, view, sem).wait()


def surface_kernel(
    groups, columns, coef_hbm, spacing_hbm, weights_hbm, basis_hbm, twiddle_hbm,
    s_out, sides, table,
    coef, spacing, weights, basis, twiddle, turned, gathered, operand,
    product_one, product_two, landed_one, landed_two, landed_sides, best, bests, partial,
    load_sem, send_one, recv_one, send_two, recv_two, send_side, recv_side,
    send_max, recv_max, later_sem,
):
    gx, gy = lax.axis_index("gx"), lax.axis_index("gy")
    cores, rows_of = 2, groups // 2

    def other(d):
        core = lax.rem(gx + d % cores, cores)
        row = lax.rem(gx // rows_of + d // rows_of, 2)
        col = lax.rem(gx // cores + (d // cores) % 2, 2)
        return row * rows_of + col * cores + core

    peers = [other(d) for d in (6, 7, 2, 3, 4, 5, 1)]
    loads = [
        pltpu.make_async_copy(src, dst, load_sem.at[i])
        for i, (src, dst) in enumerate((
            (coef_hbm, coef),
            (spacing_hbm, spacing),
            (weights_hbm, weights),
            (twiddle_hbm, twiddle),
            (basis_hbm, basis),
        ))
    ]
    for load in loads:
        load.start()

    barrier = pltpu.get_barrier_semaphore()
    for peer in peers:
        pl.semaphore_signal(barrier, inc=1, device_id=(peer, gy), device_id_type=MESH)
    for up in range(1, columns):

        @pl.when(gy + up < columns)
        def _():
            for d in range(groups):
                target = (lax.rem(gx + d, groups), gy + up)
                pl.semaphore_signal(barrier, inc=1, device_id=target, device_id_type=MESH)

    part = coef.shape[1]
    ys = coef.shape[2] // groups
    half = NX // RADIX
    flip = gx // rows_of

    def sub_of(chunk, target):
        return lax.rem(chunk + target // rows_of, 2)

    def turned_rows(chunk, target):
        return pl.ds(pl.multiple_of(target * ys + sub_of(chunk, target) * TILE, TILE), TILE)

    loads[0].wait()
    turned[:, :part] = coef[0].T
    turned[:, part:] = coef[1].T
    pl.semaphore_wait(barrier, groups - 1 + groups * gy)

    for chunk in range(2):
        for target in peers:
            pltpu.make_async_remote_copy(
                src_ref=turned.at[turned_rows(chunk, target)],
                dst_ref=gathered.at[chunk, gx],
                send_sem=send_one,
                recv_sem=recv_one.at[chunk],
                device_id=(target, gy),
                device_id_type=MESH,
            ).start()
    for down in range(1, columns):

        @pl.when(gy >= down)
        def _():
            for d in range(groups):
                target = (lax.rem(gx + d, groups), gy - down)
                pl.semaphore_signal(later_sem, inc=1, device_id=target, device_id_type=MESH)

    for chunk in range(2):
        gathered[chunk, gx] = turned[turned_rows(chunk, gx), :]

    for load in loads[1:]:
        load.wait()
    thick = spacing[...]
    total = jnp.sum(thick, axis=1, keepdims=True)
    scale = spacing.shape[1] * 1.0
    levels = spacing.shape[1] + 1
    stretch = jnp.sum(weights[0] * thick, axis=1, keepdims=True) / total
    slope = jnp.sum(weights[1] * thick, axis=1, keepdims=True) / total
    least = jnp.min(slope, axis=0, keepdims=True)
    table[0] = jnp.broadcast_to(scale * stretch, (levels, LANES))
    table[1] = jnp.broadcast_to(scale * (1.0 - stretch), (levels, LANES))
    table[2] = jnp.broadcast_to(scale * slope, (levels, LANES))

    rows = basis.shape[0] // 2
    block = rows // groups
    own = block - TILE
    count = own * RADIX
    width = RADIX * TILE
    dot = functools.partial(
        lax.dot_general,
        dimension_numbers=(((1,), (1,)), ((), ())),
        preferred_element_type=jnp.float32,
    )

    def transform(chunk):
        values = [
            (gathered[chunk, i, :, :part], gathered[chunk, i, :, part:]) for i in range(groups)
        ]
        even = fourier(values)
        odd = fourier([rotate(v, 2.0 * math.pi * i / RADIX) for i, v in enumerate(values)])
        for r in range(0, RADIX, 2):
            pair = []
            for k, (re, im) in ((r, even[r // 2]), (r + 1, odd[r // 2])):
                if k:
                    cos, sin = twiddle[k : k + 1, :half], twiddle[k : k + 1, half:]
                    re, im = re * cos + im * sin, im * cos - re * sin
                pair.append((re, im))
            for at, lanes in enumerate((slice(0, half), slice(half, 2 * half))):
                high, low = split(jnp.concatenate([pair[0][at], pair[1][at]], axis=0))
                operand[r * TILE : (r + 2) * TILE, lanes] = high
                operand[width + r * TILE : width + (r + 2) * TILE, lanes] = low
        both = dot(basis[:rows], operand[...])
        return both[:, :width] + both[:, width:] + dot(basis[rows:], operand[:width])

    def send_product(product, landed, chunk):
        for target in peers:
            pltpu.make_async_remote_copy(
                src_ref=product.at[target],
                dst_ref=landed.at[gx],
                send_sem=send_two,
                recv_sem=recv_two.at[chunk],
                device_id=(target, gy),
                device_id_type=MESH,
            ).start()
        landed[gx] = product[gx]

    def tallest(raw):
        return functools.reduce(jnp.maximum, [raw[i : i + TILE] for i in range(0, rows, TILE)])

    arrived(gathered.at[0, pl.ds(0, groups - 1)], recv_one.at[0])
    raw = transform(0)
    ends_one = [raw[dest * block + own : (dest + 1) * block] for dest in range(groups)]
    for dest in range(groups):
        product_one[dest] = raw[dest * block : dest * block + own]
    send_product(product_one, landed_one, 0)
    peak_one = tallest(raw)

    @pl.when(gy < columns - 1)
    def _():
        pl.semaphore_wait(later_sem, groups * (columns - 1 - gy))

    for which, sender in enumerate((0, groups - 1)):

        @pl.when(gx == sender)
        def _():
            for dest in range(groups):
                pltpu.make_async_remote_copy(
                    src_ref=product_one.at[dest],
                    dst_ref=landed_sides.at[which],
                    send_sem=send_side,
                    recv_sem=recv_side.at[which],
                    device_id=(dest, lax.rem(gy + (columns - 1, 1)[which], columns)),
                    device_id_type=MESH,
                ).start()

    arrived(gathered.at[1, pl.ds(0, groups - 1)], recv_one.at[1])
    raw = transform(1)
    sublane = lax.broadcasted_iota(jnp.int32, (TILE, LANES), 0)
    for dest in range(groups):
        product_two[dest, :own] = raw[dest * block : dest * block + own]
        product_two[dest, own:] = jnp.where(
            sublane < 2, ends_one[dest], raw[dest * block + own : (dest + 1) * block]
        )
    send_product(product_two, landed_two, 1)
    best[...] = jnp.broadcast_to(
        jnp.max(jnp.maximum(peak_one, tallest(raw)), keepdims=True), (TILE, LANES)
    )
    for d in range(1, groups * columns):
        pltpu.make_async_remote_copy(
            src_ref=best,
            dst_ref=bests.at[d],
            send_sem=send_max,
            recv_sem=recv_max,
            device_id=(
                lax.rem(gx + d // columns, groups),
                lax.rem(gy + d % columns, columns),
            ),
            device_id_type=MESH,
        ).start()

    def surface(piece):
        return TOPO_SCALE * jnp.tanh(piece * 0.25)

    lane = lax.broadcasted_iota(jnp.int32, (own, LANES), 1)
    arrived(landed_one.at[pl.ds(0, groups - 1)], recv_two.at[0])
    first = {b: surface(landed_one[j]) for j, b in enumerate(blocks_of(0, groups))}
    for bit in (2, 4):
        first = butterfly(first, bit, lane)
    for b, value in first.items():
        partial[b // 2] = value

    arrived(landed_two.at[pl.ds(0, groups - 1)], recv_two.at[1])
    second = {b: surface(landed_two[j, :own]) for j, b in enumerate(blocks_of(1, groups))}
    for bit in (2, 4):
        second = butterfly(second, bit, lane)
    pieces = {b: partial[b // 2] for b in first} | second
    for bit in (8, 1):
        pieces = butterfly(pieces, bit, lane)
    for r in range(RADIX):
        s_out[pl.ds(TILE + r, own, stride=RADIX), :] = pieces[r]

    lane = lax.broadcasted_iota(jnp.int32, (TILE, LANES), 1)
    ends = {b: surface(landed_two[b // 2, own:]) for b in range(2 * groups)}
    for bit in (2, 4, 8, 1):
        ends = butterfly(ends, bit, lane)
    is_late = lax.rem(lane // TILE + lane // (LANES // 2), 2)[0:1] == 1
    for i in range(2):
        before, after = ends[RADIX - 2 + i], ends[i]
        s_out[TILE - 2 + i : TILE - 1 + i, :] = jnp.where(is_late, before[2:3], before[0:1])
        s_out[TILE + count + i : TILE + count + i + 1, :] = jnp.where(
            is_late, after[3:4], after[1:2]
        )

    for which in range(2):
        arrived(landed_sides.at[which], recv_side.at[which])
        sides[which] = surface(landed_sides[which])

    arrived(turned.at[pl.ds(0, (groups - 1) * ys)], send_one)
    arrived(product_one.at[pl.ds(0, groups - 1)], send_two)
    arrived(product_two.at[pl.ds(0, groups - 1)], send_two)

    @pl.when(jnp.logical_or(gx == 0, gx == groups - 1))
    def _():
        arrived(product_one, send_side)

    arrived(bests.at[pl.ds(1, groups * columns - 1)], recv_max)
    arrived(bests.at[pl.ds(1, groups * columns - 1)], send_max)
    peak = best[0:1, :]
    for d in range(1, groups * columns):
        peak = jnp.maximum(peak, bests[d, 0:1, :])
    table[3] = jnp.broadcast_to(slope, (levels, LANES)) / ((1.0 - surface(peak)) * least)


def surface_by_kernel(coefficients, spacing, groups, columns):
    _, modes, ys = coefficients.shape
    full, twiddle, block = transform_tables(modes * groups, groups)
    high = full.astype(jnp.bfloat16)
    low = (full - high.astype(np.float32)).astype(jnp.bfloat16)
    basis = np.concatenate([high, low], axis=0)
    weights = level_weights(spacing.shape[0])
    levels = spacing.shape[0] + 1
    count = NX // groups
    own = block - TILE
    width = RADIX * TILE
    vmem = pl.BlockSpec(memory_space=pltpu.VMEM)
    hbm = pl.BlockSpec(memory_space=pltpu.HBM)
    dma = pltpu.SemaphoreType.DMA
    f32 = jnp.float32
    return pl.pallas_call(
        functools.partial(surface_kernel, groups, columns),
        out_shape=(
            pltpu.VMEM((count + 2 * TILE, ys), f32),
            pltpu.VMEM((2, own, LANES), f32),
            pltpu.VMEM((4, levels, LANES), f32),
        ),
        in_specs=[hbm] * 5,
        out_specs=(vmem,) * 3,
        scratch_shapes=[
            pltpu.VMEM(coefficients.shape, f32),
            pltpu.VMEM((1, spacing.shape[0]), f32),
            pltpu.VMEM(weights.shape, f32),
            pltpu.VMEM(basis.shape, jnp.bfloat16),
            pltpu.VMEM(twiddle.shape, f32),
            pltpu.VMEM((ys, 2 * modes), f32),
            pltpu.VMEM((2, groups, TILE, 2 * modes), f32),
            pltpu.VMEM((2 * width, 2 * modes), jnp.bfloat16),
            pltpu.VMEM((groups, own, LANES), f32),
            pltpu.VMEM((groups, block, LANES), f32),
            pltpu.VMEM((groups, own, LANES), f32),
            pltpu.VMEM((groups, block, LANES), f32),
            pltpu.VMEM((2, own, LANES), f32),
            pltpu.VMEM((TILE, LANES), f32),
            pltpu.VMEM((groups * columns, TILE, LANES), f32),
            pltpu.VMEM((groups, own, LANES), f32),
            dma((5,)),
            dma(()),
            dma((2,)),
            dma(()),
            dma((2,)),
            dma(()),
            dma((2,)),
            dma(()),
            dma(()),
            pltpu.SemaphoreType.REGULAR,
        ],
        compiler_params=pltpu.CompilerParams(
            collective_id=0, has_side_effects=True, vmem_limit_bytes=12 << 20
        ),
    )(*[
        pltpu.with_memory_space_constraint(jnp.asarray(x), pltpu.HBM)
        for x in (coefficients, spacing[None], weights, basis, twiddle)
    ])


def surface_by_gather(coefficients, spacing, groups):
    x_count = NX // groups
    x_first = lax.axis_index("gx") * x_count
    x_cells = x_first + jnp.arange(x_count, dtype=jnp.int32)
    portion = lax.all_gather(coefficients, "gx", axis=1, tiled=True)
    cosine, sine = basis(portion.shape[1], x_cells)
    surface = TOPO_SCALE * jnp.tanh(project(cosine, sine, portion) * 0.25)
    stretch = stretching(spacing)
    scale = stretch.shape[0] - 1.0
    slope = vertical(stretch)
    peak = lax.pmax(jnp.max(surface), ("gx", "gy"))
    wide = extended(surface, (("gx", 0), ("gy", 1)), 2)
    dx = (8.0 * (wide[3:-1] - wide[1:-3]) - (wide[4:] - wide[:-4]))[:, 2:-2] / 12.0
    dy = (8.0 * (wide[:, 3:-1] - wide[:, 1:-3]) - (wide[:, 4:] - wide[:, :-4]))[2:-2] / 12.0
    rows = [scale * stretch, scale * (1.0 - stretch), scale * slope]
    rows.append(slope / ((1.0 - peak) * jnp.min(slope)))
    table = jnp.broadcast_to(jnp.stack(rows)[:, :, None], (4, stretch.shape[0], LANES))
    return surface, dx, dy, table


def levels_kernel(depth, s_ref, dx_ref, dy_ref, table, z_ref, slopes_ref, jac_ref, quality_ref):
    first = pl.program_id(0) * depth

    def row(which, level):
        return table[which, pl.ds(first + level, 1), :]

    for level in range(depth):
        s, gain = s_ref[...], row(1, level)
        z_ref[level] = row(0, level) + gain * s
        slopes_ref[0, level] = gain * dx_ref[...]
        slopes_ref[1, level] = gain * dy_ref[...]
        rest = 1.0 - s
        jac_ref[level] = row(2, level) * rest
        quality_ref[level] = row(3, level) * rest


def all_levels(s, dx, dy, table):
    levels = table.shape[1]
    rows, columns = s.shape
    depth = 2
    plane = pl.BlockSpec((rows, columns), lambda i: (0, 0))
    field = pl.BlockSpec((depth, rows, columns), lambda i: (i, 0, 0))
    shape = jax.ShapeDtypeStruct((levels, rows, columns), jnp.float32)
    return pl.pallas_call(
        functools.partial(levels_kernel, depth),
        grid=(levels // depth,),
        in_specs=[plane, plane, plane, pl.BlockSpec(table.shape, lambda i: (0, 0, 0))],
        out_specs=(
            field,
            pl.BlockSpec((2, depth, rows, columns), lambda i: (0, i, 0, 0)),
            field,
            field,
        ),
        out_shape=(
            shape,
            jax.ShapeDtypeStruct((2, levels, rows, columns), jnp.float32),
            shape,
            shape,
        ),
    )(s, dx, dy, table)


def write_kernel(
    s_ref, sides, table, z_hbm, slopes_hbm, jac_hbm, quality_hbm,
    z, slopes, jac, quality, dx, dy, outer, sems,
):
    levels, count, _ = z.shape
    own = sides.shape[1]
    inner = pl.ds(TILE, count)

    def row(which, level):
        return table[which, pl.ds(level, 1), :]

    def heights(level, carry):
        s = s_ref[inner, :]
        z[level] = row(0, level) + row(1, level) * s
        pltpu.make_async_copy(z.at[level], z_hbm.at[level], sems.at[0]).start()
        rest = 1.0 - s
        jac[level] = row(2, level) * rest
        pltpu.make_async_copy(jac.at[level], jac_hbm.at[level], sems.at[2]).start()
        quality[level] = row(3, level) * rest
        pltpu.make_async_copy(quality.at[level], quality_hbm.at[level], sems.at[3]).start()
        return carry

    lax.fori_loop(0, levels, heights, 0)

    def near(by):
        return s_ref[pl.ds(TILE + by, count), :]

    dx[...] = (8.0 * (near(1) - near(-1)) - (near(2) - near(-2))) * (1.0 / 12.0)
    lane = lax.broadcasted_iota(jnp.int32, (own, LANES), 1)
    for r in range(RADIX):
        right, left = sides[0], sides[1]
        if r:
            right = pltpu.roll(right, LANES - r * TILE, 1)
        if r != RADIX - 1:
            left = pltpu.roll(left, LANES - TILE - r * TILE, 1)
        outer[pl.ds(r, own, stride=RADIX), :] = jnp.where(lane < LANES // 2, right, left)
    s, edge = s_ref[inner, :], outer[...]
    lane = lax.broadcasted_iota(jnp.int32, (count, LANES), 1)

    def moved(by):
        taken = lane < by if by > 0 else lane >= LANES + by
        return pltpu.roll(jnp.where(taken, edge, s), (LANES - by) % LANES, 1)

    dy[...] = (8.0 * (moved(1) - moved(-1)) - (moved(2) - moved(-2))) * (1.0 / 12.0)

    def tilts(level, carry):
        gain = row(1, level)
        for at, slope in enumerate((dx, dy)):
            slopes[at, level] = gain * slope[...]
            pltpu.make_async_copy(
                slopes.at[at, level], slopes_hbm.at[at, level], sems.at[1]
            ).start()
        return carry

    lax.fori_loop(0, levels, tilts, 0)
    for i, (src, dst) in enumerate(
        ((z, z_hbm), (slopes, slopes_hbm), (jac, jac_hbm), (quality, quality_hbm))
    ):
        pltpu.make_async_copy(src, dst, sems.at[i]).wait()


def write_all(s, sides, table):
    levels = table.shape[1]
    count, columns = s.shape[0] - 2 * TILE, s.shape[1]
    vmem = pl.BlockSpec(memory_space=pltpu.VMEM)
    hbm = pl.BlockSpec(memory_space=pl.ANY)
    field = (levels, count, columns)
    fields = (field, (2,) + field, field, field)
    f32 = jnp.float32
    plane = pltpu.VMEM((count, columns), f32)
    return pl.pallas_call(
        write_kernel,
        in_specs=[vmem] * 3,
        out_specs=(hbm,) * 4,
        out_shape=tuple(jax.ShapeDtypeStruct(shape, f32) for shape in fields),
        scratch_shapes=[pltpu.VMEM(shape, f32) for shape in fields]
        + [plane, plane, plane, pltpu.SemaphoreType.DMA((4,))],
        compiler_params=pltpu.CompilerParams(vmem_limit_bytes=48 << 20),
    )(s, sides, table)


def shards(coefficients, spacing):
    groups, columns = lax.axis_size("gx"), lax.axis_size("gy")
    _, modes, ys = coefficients.shape
    fits = (
        groups == 8
        and ys == LANES
        and ys == groups * RADIX
        and modes == NX // RADIX
        and modes % LANES == 0
        and columns > 1
    )
    if fits:
        return write_all(*surface_by_kernel(coefficients, spacing, groups, columns))
    return all_levels(*surface_by_gather(coefficients, spacing, groups))


def solution(mesh):
    return jax.shard_map(
        shards,
        mesh=mesh,
        in_specs=(P(None, "gx", "gy"), P()),
        out_specs=(
            P(None, "gx", "gy"),
            P(None, None, "gx", "gy"),
            P(None, "gx", "gy"),
            P(None, "gx", "gy"),
        ),
        check_vma=False,
    )
```

```python
import functools
import math

import jax
import jax.numpy as jnp
import numpy as np
from jax import lax
from jax.experimental import pallas as pl
from jax.experimental.pallas import tpu as pltpu
from jax.sharding import PartitionSpec as P

NX = 4096


BOUNDARY = (
    (-24.0 / 17.0, 59.0 / 34.0, -4.0 / 17.0, -3.0 / 34.0, 0.0, 0.0),
    (-0.5, 0.0, 0.5, 0.0, 0.0, 0.0),
    (4.0 / 43.0, -59.0 / 86.0, 0.0, 59.0 / 86.0, -4.0 / 43.0, 0.0),
    (3.0 / 98.0, 0.0, -59.0 / 98.0, 0.0, 32.0 / 49.0, -4.0 / 49.0),
)
TOPO_SCALE = 0.1


def extended(cells, sides, width):
    for axis, dim in sides:
        count = lax.axis_size(axis)
        head = lax.slice_in_dim(cells, 0, width, axis=dim)
        tail = lax.slice_in_dim(cells, cells.shape[dim] - width, cells.shape[dim], axis=dim)
        cells = jnp.concatenate(
            [
                lax.ppermute(tail, axis, [(i, (i + 1) % count) for i in range(count)]),
                cells,
                lax.ppermute(head, axis, [((i + 1) % count, i) for i in range(count)]),
            ],
            axis=dim,
        )
    return cells


def vertical(field):
    levels = field.shape[0]
    top_rows = []
    bottom_rows = []
    for row_id in range(4):
        upper = None
        lower = None
        for level_id, factor in enumerate(BOUNDARY[row_id]):
            if factor != 0.0:
                term_up = factor * field[level_id]
                term_down = -factor * field[levels - 1 - level_id]
                upper = term_up if upper is None else upper + term_up
                lower = term_down if lower is None else lower + term_down
        top_rows.append(upper)
        bottom_rows.append(lower)
    inner = (
        8.0 * (field[5 : levels - 3] - field[3 : levels - 5])
        - (field[6 : levels - 2] - field[2 : levels - 6])
    ) / 12.0
    return jnp.concatenate([jnp.stack(top_rows), inner, jnp.stack(bottom_rows[::-1])], axis=0)


def stretching(spacing):
    summed = jnp.sum(spacing)
    return jnp.concatenate([jnp.zeros((1,), spacing.dtype), jnp.cumsum(spacing)]) / summed


def column_depth(surface, stretch):
    levels = stretch.shape[0]
    return (levels - 1.0) * (surface[None] + (1.0 - surface[None]) * stretch[:, None, None])


def basis(count, x_cells):
    mode_ids = jnp.arange(count, dtype=jnp.int32)
    phase = (mode_ids[:, None] * x_cells[None, :] % NX).astype(jnp.float32) * (2.0 * math.pi / NX)
    return (jnp.cos(phase), jnp.sin(phase))


def project(cosine, sine, portion):
    first = jnp.dot(
        cosine.T, portion[0], precision=lax.Precision.HIGHEST, preferred_element_type=jnp.float32
    )
    return first + jnp.dot(
        sine.T, portion[1], precision=lax.Precision.HIGHEST, preferred_element_type=jnp.float32
    )


LANES = 128
RADIX = 16
TILE = 8
MESH = pl.DeviceIdType.MESH


def level_weights(gaps):
    levels = gaps + 1
    summed = np.tril(np.ones((levels, gaps)), -1)
    deriv = np.zeros((levels, levels))
    for row in range(levels):
        if row < 4:
            deriv[row, :6] = BOUNDARY[row]
        elif row >= levels - 4:
            deriv[row, ::-1][:6] = -np.array(BOUNDARY[levels - 1 - row])
        else:
            deriv[row, row - 2 : row + 3] = np.array([1.0, -8.0, 0.0, 8.0, -1.0]) / 12.0
    return np.stack([summed, deriv @ summed]).astype(np.float32)


def transform_tables():
    part = NX // RADIX
    angle = 2.0 * np.pi / part * ((np.arange(part)[:, None] * np.arange(part)[None]) % part)
    full = np.concatenate([np.cos(angle), np.sin(angle)], axis=1).astype(np.float32)
    turn = 2.0 * np.pi / NX * (np.arange(RADIX)[:, None] * np.arange(part)[None])
    twiddle = np.concatenate([np.cos(turn), np.sin(turn)], axis=1).astype(np.float32)
    return full, twiddle


def rotate(value, angle):
    re, im = value
    cos, sin = math.cos(angle), math.sin(angle)
    if abs(sin) < 1e-12:
        return (re, im) if cos > 0 else (-re, -im)
    if abs(cos) < 1e-12:
        return (im, -re) if sin > 0 else (-im, re)
    if abs(abs(cos) - abs(sin)) < 1e-12:
        unit = math.sqrt(0.5)
        a, b = math.copysign(1.0, cos), math.copysign(1.0, sin)
        one = re * unit if a > 0 else re * -unit
        two = im * unit if a > 0 else im * -unit
        if a == b:
            return one + two, two - one
        return one - two, two + one
    return re * cos + im * sin, im * cos - re * sin


def fourier(values):
    count = len(values)
    if count == 1:
        return values
    even, odd = fourier(values[0::2]), fourier(values[1::2])
    out = [None] * count
    for i in range(count // 2):
        re, im = rotate(odd[i], 2.0 * math.pi * i / count)
        out[i] = (even[i][0] + re, even[i][1] + im)
        out[i + count // 2] = (even[i][0] - re, even[i][1] - im)
    return out


def split(value):
    high = value.astype(jnp.bfloat16)
    return high, (value - high.astype(jnp.float32)).astype(jnp.bfloat16)


def butterfly(values, bit, lane):
    shift = bit * TILE
    upper = (lane // TILE) & bit != 0
    for i in sorted(values):
        if not i & bit and i | bit in values:
            low, high = values[i], values[i | bit]
            values[i] = jnp.where(upper, pltpu.roll(high, shift, 1), low)
            values[i | bit] = jnp.where(upper, high, pltpu.roll(low, LANES - shift, 1))
    return values


def blocks_of(chunk, groups):
    return [2 * j + (chunk + j // (groups // 2)) % 2 for j in range(groups)]


def surface(raw):
    return TOPO_SCALE * jnp.tanh(raw * 0.25)


def arrived(view, sem):
    pltpu.make_async_copy(view, view, sem).wait()


def surface_kernel(
    groups, columns, coef_hbm, spacing_hbm, weights_hbm, basis_hbm, twiddle_hbm,
    s_out, sides, table, peak_out,
    coef, spacing, weights, basis, twiddle, turned, gathered, operand,
    product_one, product_two, landed_one, landed_two, ends, landed_ends,
    side_parts, landed_sides, best, bests, partial,
    load_sem, send_one, recv_one, send_two, recv_two, send_ends, recv_ends,
    send_side, recv_side, send_max, recv_max, later_sem,
):
    gx, gy = lax.axis_index("gx"), lax.axis_index("gy")
    cores, rows_of = 2, groups // 2

    def other(d):
        core = lax.rem(gx + d % cores, cores)
        row = lax.rem(gx // rows_of + d // rows_of, 2)
        col = lax.rem(gx // cores + (d // cores) % 2, 2)
        return row * rows_of + col * cores + core

    peers = [other(d) for d in (6, 7, 2, 3, 4, 5, 1)]
    loads = [
        pltpu.make_async_copy(src, dst, load_sem.at[i])
        for i, (src, dst) in enumerate((
            (coef_hbm, coef),
            (spacing_hbm, spacing),
            (weights_hbm, weights),
            (twiddle_hbm, twiddle),
            (basis_hbm, basis),
        ))
    ]
    loads[0].start()
    barrier = pltpu.get_barrier_semaphore()
    for peer in peers:
        pl.semaphore_signal(barrier, inc=1, device_id=(peer, gy), device_id_type=MESH)
    for up in range(1, columns):

        @pl.when(gy + up < columns)
        def _():
            for d in range(groups):
                target = (lax.rem(gx + d, groups), gy + up)
                pl.semaphore_signal(barrier, inc=1, device_id=target, device_id_type=MESH)

    part = coef.shape[1]
    ys = coef.shape[2] // groups
    half = NX // RADIX
    flip = gx // rows_of

    def sub_of(chunk, target):
        return lax.rem(chunk + target // rows_of, 2)

    def turned_rows(chunk, target):
        return pl.ds(pl.multiple_of(target * ys + sub_of(chunk, target) * TILE, TILE), TILE)

    loads[0].wait()
    for load in loads[1:]:
        load.start()
    turned[:, :part] = coef[0].T
    turned[:, part:] = coef[1].T
    pl.semaphore_wait(barrier, groups - 1 + groups * gy)

    for chunk in range(2):
        for target in peers:
            pltpu.make_async_remote_copy(
                src_ref=turned.at[turned_rows(chunk, target)],
                dst_ref=gathered.at[chunk, gx],
                send_sem=send_one,
                recv_sem=recv_one.at[chunk],
                device_id=(target, gy),
                device_id_type=MESH,
            ).start()
    for down in range(1, columns):

        @pl.when(gy >= down)
        def _():
            for d in range(groups):
                target = (lax.rem(gx + d, groups), gy - down)
                pl.semaphore_signal(later_sem, inc=1, device_id=target, device_id_type=MESH)

    for chunk in range(2):
        gathered[chunk, gx] = turned[turned_rows(chunk, gx), :]

    for load in loads[1:]:
        load.wait()
    thick = spacing[...]
    total = jnp.sum(thick, axis=1, keepdims=True)
    scale = spacing.shape[1] * 1.0
    levels = spacing.shape[1] + 1
    stretch = jnp.sum(weights[0] * thick, axis=1, keepdims=True) / total
    slope = jnp.sum(weights[1] * thick, axis=1, keepdims=True) / total
    least = jnp.min(slope, axis=0, keepdims=True)
    table[0] = jnp.broadcast_to(scale * stretch, (levels, LANES))
    table[1] = jnp.broadcast_to(scale * (1.0 - stretch), (levels, LANES))
    table[2] = jnp.broadcast_to(scale * slope, (levels, LANES))
    table[3] = jnp.broadcast_to(slope / least, (levels, LANES))

    rows = basis.shape[0] // 2
    own = rows // groups
    count = own * RADIX
    width = RADIX * TILE
    dot = functools.partial(
        lax.dot_general,
        dimension_numbers=(((1,), (1,)), ((), ())),
        preferred_element_type=jnp.float32,
    )

    def transform(chunk):
        values = [
            (gathered[chunk, i, :, :part], gathered[chunk, i, :, part:]) for i in range(groups)
        ]
        even = fourier(values)
        odd = fourier([rotate(v, 2.0 * math.pi * i / RADIX) for i, v in enumerate(values)])
        for r in range(0, RADIX, 2):
            pair = []
            for k, (re, im) in ((r, even[r // 2]), (r + 1, odd[r // 2])):
                if k:
                    cos, sin = twiddle[k : k + 1, :half], twiddle[k : k + 1, half:]
                    re, im = re * cos + im * sin, im * cos - re * sin
                pair.append((re, im))
            for at, lanes in enumerate((slice(0, half), slice(half, 2 * half))):
                high, low = split(jnp.concatenate([pair[0][at], pair[1][at]], axis=0))
                operand[r * TILE : (r + 2) * TILE, lanes] = high
                operand[width + r * TILE : width + (r + 2) * TILE, lanes] = low
        both = dot(basis[:rows], operand[...])
        return both[:, :width] + both[:, width:] + dot(basis[rows:], operand[:width])

    def send_product(product, landed, chunk):
        for target in peers:
            pltpu.make_async_remote_copy(
                src_ref=product.at[target],
                dst_ref=landed.at[gx],
                send_sem=send_two,
                recv_sem=recv_two.at[chunk],
                device_id=(target, gy),
                device_id_type=MESH,
            ).start()
        landed[gx] = product[gx]

    def tallest(raw):
        return functools.reduce(jnp.maximum, [raw[i : i + TILE] for i in range(0, rows, TILE)])

    row_lane = lax.broadcasted_iota(jnp.int32, (1, LANES), 1)

    def ends_of(raw):
        return [
            jnp.where(
                row_lane < LANES // 2,
                raw[(dest + 1) * own % rows : (dest + 1) * own % rows + 1],
                raw[(dest * own - 1) % rows : (dest * own - 1) % rows + 1],
            )
            for dest in range(groups)
        ]

    def send_best(target, slot):
        for d in range(groups):
            pltpu.make_async_remote_copy(
                src_ref=best,
                dst_ref=bests.at[slot * groups + gx],
                send_sem=send_max,
                recv_sem=recv_max,
                device_id=(lax.rem(gx + d, groups), target),
                device_id_type=MESH,
            ).start()

    lane_one = lax.broadcasted_iota(jnp.int32, (TILE, LANES), 1)

    def pack_sides(which):
        for dest in range(groups):
            packed = None
            for k in range(own // TILE):
                shift = (2 * k - which * (TILE - 2)) % LANES
                tile = product_one[dest, k * TILE : (k + 1) * TILE]
                tile = pltpu.roll(tile, shift, 1) if shift else tile
                packed = tile if k == 0 else jnp.where(lane_one % TILE // 2 == k, tile, packed)
            side_parts[dest] = packed

    def send_sides(to_lower):
        for which, sender in enumerate((0, groups - 1)):
            column = lax.rem(gy + (columns - 1, 1)[which], columns)

            @pl.when(jnp.logical_and(gx == sender, (column < gy) if to_lower else (column > gy)))
            def _():
                for dest in range(groups):
                    pltpu.make_async_remote_copy(
                        src_ref=side_parts.at[dest],
                        dst_ref=landed_sides.at[which],
                        send_sem=send_side,
                        recv_sem=recv_side.at[which],
                        device_id=(dest, column),
                        device_id_type=MESH,
                    ).start()

    arrived(gathered.at[0, pl.ds(0, groups - 1)], recv_one.at[0])
    raw = transform(0)
    for dest in range(groups):
        product_one[dest] = raw[dest * own : (dest + 1) * own]
    send_product(product_one, landed_one, 0)
    ends_one = ends_of(raw)
    peak_one = tallest(raw)

    for which, sender in enumerate((0, groups - 1)):
        pl.when(gx == sender)(functools.partial(pack_sides, which))
    send_sides(True)

    arrived(gathered.at[1, pl.ds(0, groups - 1)], recv_one.at[1])
    raw = transform(1)
    for dest in range(groups):
        product_two[dest] = raw[dest * own : (dest + 1) * own]
    best[...] = jnp.max(jnp.maximum(peak_one, tallest(raw)), axis=0, keepdims=True)
    for down in range(columns - 1, 0, -1):

        @pl.when(gy >= down)
        def _():
            send_best(gy - down, down - 1)

    send_product(product_two, landed_two, 1)
    ends_two = ends_of(raw)
    outside = jnp.abs(row_lane // TILE * 2 - (RADIX - 1)) > RADIX // 2
    for dest in range(groups):
        one, two = ends_one[dest], ends_two[dest]
        low, high = jnp.where(flip == 0, one, two), jnp.where(flip == 0, two, one)
        ends[dest, 0:1] = jnp.where(outside, low, pltpu.roll(high, LANES // 2, 1))
        ends[dest, 1:2] = best[...]
    for target in peers:
        pltpu.make_async_remote_copy(
            src_ref=ends.at[target],
            dst_ref=landed_ends.at[gx],
            send_sem=send_ends,
            recv_sem=recv_ends,
            device_id=(target, gy),
            device_id_type=MESH,
        ).start()
    landed_ends[gx] = ends[gx]

    @pl.when(gy < columns - 1)
    def _():
        pl.semaphore_wait(later_sem, groups * (columns - 1 - gy))

    send_sides(False)

    for up in range(1, columns):

        @pl.when(gy + up < columns)
        def _():
            send_best(gy + up, columns - up - 1)

    lane = lax.broadcasted_iota(jnp.int32, (own, LANES), 1)
    arrived(landed_one.at[pl.ds(0, groups - 1)], recv_two.at[0])
    first = {b: surface(landed_one[j]) for j, b in enumerate(blocks_of(0, groups))}
    for bit in (2, 4):
        first = butterfly(first, bit, lane)
    for b, value in first.items():
        partial[b // 2] = value

    arrived(landed_two.at[pl.ds(0, groups - 1)], recv_two.at[1])
    second = {b: surface(landed_two[j]) for j, b in enumerate(blocks_of(1, groups))}
    for bit in (2, 4):
        second = butterfly(second, bit, lane)
    pieces = {b: partial[b // 2] for b in first} | second
    for bit in (8, 1):
        pieces = butterfly(pieces, bit, lane)
    for r in range(RADIX):
        s_out[pl.ds(TILE + r, own, stride=RADIX), :] = pieces[r]

    arrived(landed_ends.at[pl.ds(0, groups - 1)], recv_ends)
    edge = pltpu.roll(surface(landed_ends[:, 0, :]), 0, 1, stride=2 * TILE, stride_axis=0)
    lane = lax.broadcasted_iota(jnp.int32, (groups, LANES), 1)
    source = lax.broadcasted_iota(jnp.int32, (groups, LANES), 0)
    for at, r in ((-2, RADIX - 2), (-1, RADIX - 1), (count, 0), (count + 1, 1)):
        total_row = None
        for sub in range(2):
            shift = (sub - (r - sub * RADIX // 2)) * TILE % LANES
            moved = pltpu.roll(edge, shift, 1) if shift else edge
            moved = jnp.where(lane // TILE == 2 * source + sub, moved, 0.0)
            total_row = moved if sub == 0 else total_row + moved
        s_out[TILE + at : TILE + at + 1, :] = jnp.sum(total_row, axis=0, keepdims=True)

    for which in range(2):
        arrived(landed_sides.at[which], recv_side.at[which])
        sides[which] = surface(landed_sides[which])

    arrived(turned.at[pl.ds(0, (groups - 1) * ys)], send_one)
    arrived(product_one.at[pl.ds(0, groups - 1)], send_two)
    arrived(product_two.at[pl.ds(0, groups - 1)], send_two)
    arrived(ends.at[pl.ds(0, groups - 1)], send_ends)

    @pl.when(jnp.logical_or(gx == 0, gx == groups - 1))
    def _():
        arrived(side_parts, send_side)

    arrived(bests, recv_max)
    arrived(bests, send_max)
    peak = jnp.max(landed_ends[:, 1, :], axis=0, keepdims=True)
    for d in range(groups * (columns - 1)):
        peak = jnp.maximum(peak, bests[d])
    peak_out[...] = peak


def surface_by_kernel(coefficients, spacing, groups, columns):
    _, modes, ys = coefficients.shape
    full, twiddle = transform_tables()
    high = full.astype(jnp.bfloat16)
    low = (full - high.astype(np.float32)).astype(jnp.bfloat16)
    basis = np.concatenate([high, low], axis=0)
    weights = level_weights(spacing.shape[0])
    levels = spacing.shape[0] + 1
    count = NX // groups
    own = count // RADIX
    width = RADIX * TILE
    vmem = pl.BlockSpec(memory_space=pltpu.VMEM)
    hbm = pl.BlockSpec(memory_space=pltpu.HBM)
    dma = pltpu.SemaphoreType.DMA
    f32 = jnp.float32
    return pl.pallas_call(
        functools.partial(surface_kernel, groups, columns),
        out_shape=(
            pltpu.VMEM((count + 2 * TILE, ys), f32),
            pltpu.VMEM((2, TILE, LANES), f32),
            pltpu.VMEM((4, levels, LANES), f32),
            pltpu.VMEM((1, LANES), f32),
        ),
        in_specs=[hbm] * 5,
        out_specs=(vmem,) * 4,
        scratch_shapes=[
            pltpu.VMEM(coefficients.shape, f32),
            pltpu.VMEM((1, spacing.shape[0]), f32),
            pltpu.VMEM(weights.shape, f32),
            pltpu.VMEM(basis.shape, jnp.bfloat16),
            pltpu.VMEM(twiddle.shape, f32),
            pltpu.VMEM((ys, 2 * modes), f32),
            pltpu.VMEM((2, groups, TILE, 2 * modes), f32),
            pltpu.VMEM((2 * width, 2 * modes), jnp.bfloat16),
        ]
        + [pltpu.VMEM((groups, own, LANES), f32)] * 4
        + [
            pltpu.VMEM((groups, 2, LANES), f32),
            pltpu.VMEM((groups, 2, LANES), f32),
            pltpu.VMEM((groups, TILE, LANES), f32),
            pltpu.VMEM((2, TILE, LANES), f32),
            pltpu.VMEM((1, LANES), f32),
            pltpu.VMEM((groups * (columns - 1), 1, LANES), f32),
            pltpu.VMEM((groups, own, LANES), f32),
            dma((5,)),
            dma(()),
            dma((2,)),
            dma(()),
            dma((2,)),
            dma(()),
            dma(()),
            dma(()),
            dma((2,)),
            dma(()),
            dma(()),
            pltpu.SemaphoreType.REGULAR,
        ],
        compiler_params=pltpu.CompilerParams(
            collective_id=0, has_side_effects=True, vmem_limit_bytes=12 << 20
        ),
    )(*[
        pltpu.with_memory_space_constraint(jnp.asarray(x), pltpu.HBM)
        for x in (coefficients, spacing[None], weights, basis, twiddle)
    ])


def surface_by_gather(coefficients, spacing, groups):
    x_count = NX // groups
    x_first = lax.axis_index("gx") * x_count
    x_cells = x_first + jnp.arange(x_count, dtype=jnp.int32)
    portion = lax.all_gather(coefficients, "gx", axis=1, tiled=True)
    cosine, sine = basis(portion.shape[1], x_cells)
    surface = TOPO_SCALE * jnp.tanh(project(cosine, sine, portion) * 0.25)
    stretch = stretching(spacing)
    scale = stretch.shape[0] - 1.0
    slope = vertical(stretch)
    peak = lax.pmax(jnp.max(surface), ("gx", "gy"))
    wide = extended(surface, (("gx", 0), ("gy", 1)), 2)
    dx = (8.0 * (wide[3:-1] - wide[1:-3]) - (wide[4:] - wide[:-4]))[:, 2:-2] / 12.0
    dy = (8.0 * (wide[:, 3:-1] - wide[:, 1:-3]) - (wide[:, 4:] - wide[:, :-4]))[2:-2] / 12.0
    rows = [scale * stretch, scale * (1.0 - stretch), scale * slope]
    rows.append(slope / ((1.0 - peak) * jnp.min(slope)))
    table = jnp.broadcast_to(jnp.stack(rows)[:, :, None], (4, stretch.shape[0], LANES))
    return surface, dx, dy, table


def levels_kernel(depth, s_ref, dx_ref, dy_ref, table, z_ref, slopes_ref, jac_ref, quality_ref):
    first = pl.program_id(0) * depth

    def row(which, level):
        return table[which, pl.ds(first + level, 1), :]

    for level in range(depth):
        s, gain = s_ref[...], row(1, level)
        z_ref[level] = row(0, level) + gain * s
        slopes_ref[0, level] = gain * dx_ref[...]
        slopes_ref[1, level] = gain * dy_ref[...]
        rest = 1.0 - s
        jac_ref[level] = row(2, level) * rest
        quality_ref[level] = row(3, level) * rest


def all_levels(s, dx, dy, table):
    levels = table.shape[1]
    rows, columns = s.shape
    depth = 2
    plane = pl.BlockSpec((rows, columns), lambda i: (0, 0))
    field = pl.BlockSpec((depth, rows, columns), lambda i: (i, 0, 0))
    shape = jax.ShapeDtypeStruct((levels, rows, columns), jnp.float32)
    return pl.pallas_call(
        functools.partial(levels_kernel, depth),
        grid=(levels // depth,),
        in_specs=[plane, plane, plane, pl.BlockSpec(table.shape, lambda i: (0, 0, 0))],
        out_specs=(
            field,
            pl.BlockSpec((2, depth, rows, columns), lambda i: (0, i, 0, 0)),
            field,
            field,
        ),
        out_shape=(
            shape,
            jax.ShapeDtypeStruct((2, levels, rows, columns), jnp.float32),
            shape,
            shape,
        ),
    )(s, dx, dy, table)


def write_kernel(
    s_ref, sides, table, peak, z_hbm, slopes_hbm, jac_hbm, quality_hbm,
    z, slopes, jac, quality, dx, dy, outer, scaled, sems,
):
    levels, count, _ = z.shape
    own = count // RADIX
    inner = pl.ds(TILE, count)

    def row(which, level):
        return table[which, pl.ds(level, 1), :]

    def put(src, dst, at, which):
        pltpu.make_async_copy(src.at[at], dst.at[at], sems.at[which]).start()

    def heights(level, carry):
        s = s_ref[inner, :]
        z[level] = row(0, level) + row(1, level) * s
        put(z, z_hbm, level, 0)
        jac[level] = row(2, level) * (1.0 - s)
        put(jac, jac_hbm, level, 2)
        return carry

    lax.fori_loop(0, levels, heights, 0)
    highest = surface(jnp.max(peak[...], axis=1, keepdims=True))
    scaled[...] = table[3] / (1.0 - highest)

    def near(by):
        return s_ref[pl.ds(TILE + by, count), :]

    dx[...] = (8.0 * (near(1) - near(-1)) - (near(2) - near(-2))) * (1.0 / 12.0)
    lane = lax.broadcasted_iota(jnp.int32, (TILE, LANES), 1)
    for r in range(RADIX):
        for k in range(own // TILE):
            shift = LANES - r * TILE - 2 * k
            right = pltpu.roll(sides[0], shift % LANES, 1) if shift % LANES else sides[0]
            left = pltpu.roll(sides[1], (shift - 2) % LANES, 1) if (shift - 2) % LANES else sides[1]
            outer[pl.ds(k * TILE * RADIX + r, TILE, stride=RADIX), :] = jnp.where(
                lane < LANES // 2, right, left
            )
    s, edge = s_ref[inner, :], outer[...]
    lane = lax.broadcasted_iota(jnp.int32, (count, LANES), 1)

    def moved(by):
        taken = lane < by if by > 0 else lane >= LANES + by
        return pltpu.roll(jnp.where(taken, edge, s), (LANES - by) % LANES, 1)

    dy[...] = (8.0 * (moved(1) - moved(-1)) - (moved(2) - moved(-2))) * (1.0 / 12.0)

    def tilts(level, carry):
        gain = row(1, level)
        for at, slope in enumerate((dx, dy)):
            slopes[at, level] = gain * slope[...]
            put(slopes, slopes_hbm, (at, level), 1)
        quality[level] = scaled[pl.ds(level, 1), :] * (1.0 - s_ref[inner, :])
        put(quality, quality_hbm, level, 3)
        return carry

    lax.fori_loop(0, levels, tilts, 0)
    for i, (src, dst) in enumerate(
        ((z, z_hbm), (slopes, slopes_hbm), (jac, jac_hbm), (quality, quality_hbm))
    ):
        pltpu.make_async_copy(src, dst, sems.at[i]).wait()


def write_all(s, sides, table, peak):
    levels = table.shape[1]
    count, columns = s.shape[0] - 2 * TILE, s.shape[1]
    vmem = pl.BlockSpec(memory_space=pltpu.VMEM)
    hbm = pl.BlockSpec(memory_space=pl.ANY)
    field = (levels, count, columns)
    fields = (field, (2,) + field, field, field)
    f32 = jnp.float32
    plane = pltpu.VMEM((count, columns), f32)
    return pl.pallas_call(
        write_kernel,
        in_specs=[vmem] * 4,
        out_specs=(hbm,) * 4,
        out_shape=tuple(jax.ShapeDtypeStruct(shape, f32) for shape in fields),
        scratch_shapes=[pltpu.VMEM(shape, f32) for shape in fields]
        + [plane, plane, plane, pltpu.VMEM((levels, LANES), f32), pltpu.SemaphoreType.DMA((4,))],
        compiler_params=pltpu.CompilerParams(vmem_limit_bytes=48 << 20),
    )(s, sides, table, peak)


def shards(coefficients, spacing):
    groups, columns = lax.axis_size("gx"), lax.axis_size("gy")
    _, modes, ys = coefficients.shape
    fits = (
        groups == 8
        and ys == LANES
        and ys == groups * RADIX
        and modes == NX // RADIX
        and modes % LANES == 0
        and columns > 1
    )
    if fits:
        return write_all(*surface_by_kernel(coefficients, spacing, groups, columns))
    return all_levels(*surface_by_gather(coefficients, spacing, groups))


def solution(mesh):
    return jax.shard_map(
        shards,
        mesh=mesh,
        in_specs=(P(None, "gx", "gy"), P()),
        out_specs=(
            P(None, "gx", "gy"),
            P(None, None, "gx", "gy"),
            P(None, "gx", "gy"),
            P(None, "gx", "gy"),
        ),
        check_vma=False,
    )
```

```python
import functools
import math

import jax
import jax.numpy as jnp
import numpy as np
from jax import lax
from jax.experimental import pallas as pl
from jax.experimental.pallas import tpu as pltpu
from jax.sharding import PartitionSpec as P

NX = 4096


BOUNDARY = (
    (-24.0 / 17.0, 59.0 / 34.0, -4.0 / 17.0, -3.0 / 34.0, 0.0, 0.0),
    (-0.5, 0.0, 0.5, 0.0, 0.0, 0.0),
    (4.0 / 43.0, -59.0 / 86.0, 0.0, 59.0 / 86.0, -4.0 / 43.0, 0.0),
    (3.0 / 98.0, 0.0, -59.0 / 98.0, 0.0, 32.0 / 49.0, -4.0 / 49.0),
)
TOPO_SCALE = 0.1


def extended(cells, sides, width):
    for axis, dim in sides:
        count = lax.axis_size(axis)
        head = lax.slice_in_dim(cells, 0, width, axis=dim)
        tail = lax.slice_in_dim(cells, cells.shape[dim] - width, cells.shape[dim], axis=dim)
        cells = jnp.concatenate(
            [
                lax.ppermute(tail, axis, [(i, (i + 1) % count) for i in range(count)]),
                cells,
                lax.ppermute(head, axis, [((i + 1) % count, i) for i in range(count)]),
            ],
            axis=dim,
        )
    return cells


def vertical(field):
    levels = field.shape[0]
    top_rows = []
    bottom_rows = []
    for row_id in range(4):
        upper = None
        lower = None
        for level_id, factor in enumerate(BOUNDARY[row_id]):
            if factor != 0.0:
                term_up = factor * field[level_id]
                term_down = -factor * field[levels - 1 - level_id]
                upper = term_up if upper is None else upper + term_up
                lower = term_down if lower is None else lower + term_down
        top_rows.append(upper)
        bottom_rows.append(lower)
    inner = (
        8.0 * (field[5 : levels - 3] - field[3 : levels - 5])
        - (field[6 : levels - 2] - field[2 : levels - 6])
    ) / 12.0
    return jnp.concatenate([jnp.stack(top_rows), inner, jnp.stack(bottom_rows[::-1])], axis=0)


def stretching(spacing):
    summed = jnp.sum(spacing)
    return jnp.concatenate([jnp.zeros((1,), spacing.dtype), jnp.cumsum(spacing)]) / summed


def column_depth(surface, stretch):
    levels = stretch.shape[0]
    return (levels - 1.0) * (surface[None] + (1.0 - surface[None]) * stretch[:, None, None])


def basis(count, x_cells):
    mode_ids = jnp.arange(count, dtype=jnp.int32)
    phase = (mode_ids[:, None] * x_cells[None, :] % NX).astype(jnp.float32) * (2.0 * math.pi / NX)
    return (jnp.cos(phase), jnp.sin(phase))


def project(cosine, sine, portion):
    first = jnp.dot(
        cosine.T, portion[0], precision=lax.Precision.HIGHEST, preferred_element_type=jnp.float32
    )
    return first + jnp.dot(
        sine.T, portion[1], precision=lax.Precision.HIGHEST, preferred_element_type=jnp.float32
    )


LANES = 128
RADIX = 16
TILE = 8
MESH = pl.DeviceIdType.MESH


def level_weights(gaps):
    levels = gaps + 1
    summed = np.tril(np.ones((levels, gaps)), -1)
    deriv = np.zeros((levels, levels))
    for row in range(levels):
        if row < 4:
            deriv[row, :6] = BOUNDARY[row]
        elif row >= levels - 4:
            deriv[row, ::-1][:6] = -np.array(BOUNDARY[levels - 1 - row])
        else:
            deriv[row, row - 2 : row + 3] = np.array([1.0, -8.0, 0.0, 8.0, -1.0]) / 12.0
    return np.stack([summed, deriv @ summed]).astype(np.float32)


def transform_tables():
    part = NX // RADIX
    angle = 2.0 * np.pi / part * ((np.arange(part)[:, None] * np.arange(part)[None]) % part)
    full = np.concatenate([np.cos(angle), np.sin(angle)], axis=1).astype(np.float32)
    turn = 2.0 * np.pi / NX * (np.arange(RADIX)[:, None] * np.arange(part)[None])
    twiddle = np.concatenate([np.cos(turn), np.sin(turn)], axis=1).astype(np.float32)
    return full, twiddle


def rotate(value, angle):
    re, im = value
    cos, sin = math.cos(angle), math.sin(angle)
    if abs(sin) < 1e-12:
        return (re, im) if cos > 0 else (-re, -im)
    if abs(cos) < 1e-12:
        return (im, -re) if sin > 0 else (-im, re)
    if abs(abs(cos) - abs(sin)) < 1e-12:
        unit = math.sqrt(0.5)
        a, b = math.copysign(1.0, cos), math.copysign(1.0, sin)
        one = re * unit if a > 0 else re * -unit
        two = im * unit if a > 0 else im * -unit
        if a == b:
            return one + two, two - one
        return one - two, two + one
    return re * cos + im * sin, im * cos - re * sin


def fourier(values):
    count = len(values)
    if count == 1:
        return values
    even, odd = fourier(values[0::2]), fourier(values[1::2])
    out = [None] * count
    for i in range(count // 2):
        re, im = rotate(odd[i], 2.0 * math.pi * i / count)
        out[i] = (even[i][0] + re, even[i][1] + im)
        out[i + count // 2] = (even[i][0] - re, even[i][1] - im)
    return out


def split(value):
    high = value.astype(jnp.bfloat16)
    return high, (value - high.astype(jnp.float32)).astype(jnp.bfloat16)


def butterfly(values, bit, lane):
    shift = bit * TILE
    upper = (lane // TILE) & bit != 0
    for i in sorted(values):
        if not i & bit and i | bit in values:
            low, high = values[i], values[i | bit]
            values[i] = jnp.where(upper, pltpu.roll(high, shift, 1), low)
            values[i | bit] = jnp.where(upper, high, pltpu.roll(low, LANES - shift, 1))
    return values


def blocks_of(chunk, groups):
    return [2 * j + (chunk + j // (groups // 2)) % 2 for j in range(groups)]


def surface(raw):
    return TOPO_SCALE * jnp.tanh(raw * 0.25)


def arrived(view, sem):
    pltpu.make_async_copy(view, view, sem).wait()


def surface_kernel(
    groups, columns, coef_hbm, spacing_hbm, weights_hbm, basis_hbm, twiddle_hbm,
    s_out, sides, table, peak_out,
    coef, spacing, weights, basis, twiddle, turned, gathered, operand,
    product_one, product_two, landed_one, landed_two, ends, landed_ends,
    side_parts, landed_sides, best, bests, partial,
    load_sem, send_one, recv_one, send_two, recv_two, send_ends, recv_ends,
    send_side, recv_side, send_max, recv_max, later_sem,
):
    gx, gy = lax.axis_index("gx"), lax.axis_index("gy")
    cores, rows_of = 2, groups // 2

    def other(d):
        core = lax.rem(gx + d % cores, cores)
        row = lax.rem(gx // rows_of + d // rows_of, 2)
        col = lax.rem(gx // cores + (d // cores) % 2, 2)
        return row * rows_of + col * cores + core

    peers = [other(d) for d in (6, 7, 2, 3, 4, 5, 1)]
    loads = [
        pltpu.make_async_copy(src, dst, load_sem.at[i])
        for i, (src, dst) in enumerate((
            (coef_hbm, coef),
            (spacing_hbm, spacing),
            (weights_hbm, weights),
            (twiddle_hbm, twiddle),
            (basis_hbm, basis),
        ))
    ]
    loads[0].start()
    barrier = pltpu.get_barrier_semaphore()
    for peer in peers:
        pl.semaphore_signal(barrier, inc=1, device_id=(peer, gy), device_id_type=MESH)
    for up in range(1, columns):

        @pl.when(gy + up < columns)
        def _():
            for d in range(groups):
                target = (lax.rem(gx + d, groups), gy + up)
                pl.semaphore_signal(barrier, inc=1, device_id=target, device_id_type=MESH)

    part = coef.shape[1]
    ys = coef.shape[2] // groups
    half = NX // RADIX
    flip = gx // rows_of

    def sub_of(chunk, target):
        return lax.rem(chunk + target // rows_of, 2)

    def turned_rows(chunk, target):
        return pl.ds(pl.multiple_of(target * ys + sub_of(chunk, target) * TILE, TILE), TILE)

    loads[0].wait()
    for load in loads[1:]:
        load.start()
    turned[:, :part] = coef[0].T
    turned[:, part:] = coef[1].T
    pl.semaphore_wait(barrier, groups - 1 + groups * gy)

    far, close = peers[:2], peers[2:]
    order = [(chunk, peer) for some in (far, close) for chunk in range(2) for peer in some]
    for chunk, target in order:
        pltpu.make_async_remote_copy(
            src_ref=turned.at[turned_rows(chunk, target)],
            dst_ref=gathered.at[chunk, gx],
            send_sem=send_one,
            recv_sem=recv_one.at[chunk],
            device_id=(target, gy),
            device_id_type=MESH,
        ).start()
    for down in range(1, columns):

        @pl.when(gy >= down)
        def _():
            for d in range(groups):
                target = (lax.rem(gx + d, groups), gy - down)
                pl.semaphore_signal(later_sem, inc=1, device_id=target, device_id_type=MESH)

    for chunk in range(2):
        gathered[chunk, gx] = turned[turned_rows(chunk, gx), :]

    for load in loads[1:]:
        load.wait()
    thick = spacing[...]
    total = jnp.sum(thick, axis=1, keepdims=True)
    scale = spacing.shape[1] * 1.0
    levels = spacing.shape[1] + 1
    stretch = jnp.sum(weights[0] * thick, axis=1, keepdims=True) / total
    slope = jnp.sum(weights[1] * thick, axis=1, keepdims=True) / total
    least = jnp.min(slope, axis=0, keepdims=True)
    table[0] = jnp.broadcast_to(scale * stretch, (levels, LANES))
    table[1] = jnp.broadcast_to(scale * (1.0 - stretch), (levels, LANES))
    table[2] = jnp.broadcast_to(scale * slope, (levels, LANES))
    table[3] = jnp.broadcast_to(slope / least, (levels, LANES))

    rows = basis.shape[0] // 2
    own = rows // groups
    count = own * RADIX
    width = RADIX * TILE
    dot = functools.partial(
        lax.dot_general,
        dimension_numbers=(((1,), (1,)), ((), ())),
        preferred_element_type=jnp.float32,
    )

    def transform(chunk):
        values = [
            (gathered[chunk, i, :, :part], gathered[chunk, i, :, part:]) for i in range(groups)
        ]
        even = fourier(values)
        odd = fourier([rotate(v, 2.0 * math.pi * i / RADIX) for i, v in enumerate(values)])
        for r in range(0, RADIX, 2):
            pair = []
            for k, (re, im) in ((r, even[r // 2]), (r + 1, odd[r // 2])):
                if k:
                    cos, sin = twiddle[k : k + 1, :half], twiddle[k : k + 1, half:]
                    re, im = re * cos + im * sin, im * cos - re * sin
                pair.append((re, im))
            for at, lanes in enumerate((slice(0, half), slice(half, 2 * half))):
                high, low = split(jnp.concatenate([pair[0][at], pair[1][at]], axis=0))
                operand[r * TILE : (r + 2) * TILE, lanes] = high
                operand[width + r * TILE : width + (r + 2) * TILE, lanes] = low
        both = dot(basis[:rows], operand[...])
        return both[:, :width] + both[:, width:] + dot(basis[rows:], operand[:width])

    def send_product(product, landed, chunk):
        for target in peers:
            pltpu.make_async_remote_copy(
                src_ref=product.at[target],
                dst_ref=landed.at[gx],
                send_sem=send_two,
                recv_sem=recv_two.at[chunk],
                device_id=(target, gy),
                device_id_type=MESH,
            ).start()
        landed[gx] = product[gx]

    def tallest(raw):
        return functools.reduce(jnp.maximum, [raw[i : i + TILE] for i in range(0, rows, TILE)])

    row_lane = lax.broadcasted_iota(jnp.int32, (1, LANES), 1)

    def ends_of(raw):
        return [
            jnp.where(
                row_lane < LANES // 2,
                raw[(dest + 1) * own % rows : (dest + 1) * own % rows + 1],
                raw[(dest * own - 1) % rows : (dest * own - 1) % rows + 1],
            )
            for dest in range(groups)
        ]

    def send_best(target, slot):
        for d in range(groups):
            pltpu.make_async_remote_copy(
                src_ref=best,
                dst_ref=bests.at[slot * groups + gx],
                send_sem=send_max,
                recv_sem=recv_max,
                device_id=(lax.rem(gx + d, groups), target),
                device_id_type=MESH,
            ).start()

    lane_one = lax.broadcasted_iota(jnp.int32, (TILE, LANES), 1)

    def pack_sides():
        for dest in range(groups):
            packed = None
            for k in range(own // TILE):
                shift = jnp.where(flip == 0, 2 * k, (2 * k + 2 - TILE) % LANES)
                tile = pltpu.roll(product_one[dest, k * TILE : (k + 1) * TILE], shift, 1)
                packed = tile if k == 0 else jnp.where(lane_one % TILE // 2 == k, tile, packed)
            side_parts[dest] = packed

    def send_sides(to_lower):
        for which, sender in enumerate((0, groups - 1)):
            column = lax.rem(gy + (columns - 1, 1)[which], columns)

            @pl.when(jnp.logical_and(gx == sender, (column < gy) if to_lower else (column > gy)))
            def _():
                for dest in range(groups):
                    pltpu.make_async_remote_copy(
                        src_ref=side_parts.at[dest],
                        dst_ref=landed_sides.at[which],
                        send_sem=send_side,
                        recv_sem=recv_side.at[which],
                        device_id=(dest, column),
                        device_id_type=MESH,
                    ).start()

    arrived(gathered.at[0, pl.ds(0, groups - 1)], recv_one.at[0])
    raw = transform(0)
    for dest in range(groups):
        product_one[dest] = raw[dest * own : (dest + 1) * own]
    send_product(product_one, landed_one, 0)
    ends_one = ends_of(raw)
    peak_one = tallest(raw)

    arrived(gathered.at[1, pl.ds(0, groups - 1)], recv_one.at[1])
    raw = transform(1)
    for dest in range(groups):
        product_two[dest] = raw[dest * own : (dest + 1) * own]
    pack_sides()
    best[...] = jnp.max(jnp.maximum(peak_one, tallest(raw)), axis=0, keepdims=True)
    for down in range(columns - 1, 0, -1):

        @pl.when(gy >= down)
        def _():
            send_best(gy - down, down - 1)

        if down == columns - 1:
            send_sides(True)

    send_product(product_two, landed_two, 1)
    ends_two = ends_of(raw)
    outside = jnp.abs(row_lane // TILE * 2 - (RADIX - 1)) > RADIX // 2
    for dest in range(groups):
        one, two = ends_one[dest], ends_two[dest]
        low, high = jnp.where(flip == 0, one, two), jnp.where(flip == 0, two, one)
        ends[dest, 0:1] = jnp.where(outside, low, pltpu.roll(high, LANES // 2, 1))
        ends[dest, 1:2] = best[...]
    for target in peers:
        pltpu.make_async_remote_copy(
            src_ref=ends.at[target],
            dst_ref=landed_ends.at[gx],
            send_sem=send_ends,
            recv_sem=recv_ends,
            device_id=(target, gy),
            device_id_type=MESH,
        ).start()
    landed_ends[gx] = ends[gx]

    @pl.when(gy < columns - 1)
    def _():
        pl.semaphore_wait(later_sem, groups * (columns - 1 - gy))

    send_sides(False)

    for up in range(1, columns):

        @pl.when(gy + up < columns)
        def _():
            send_best(gy + up, columns - up - 1)

    lane = lax.broadcasted_iota(jnp.int32, (own, LANES), 1)
    arrived(landed_one.at[pl.ds(0, groups - 1)], recv_two.at[0])
    first = {b: surface(landed_one[j]) for j, b in enumerate(blocks_of(0, groups))}
    for bit in (2, 4):
        first = butterfly(first, bit, lane)
    for b, value in first.items():
        partial[b // 2] = value

    arrived(landed_two.at[pl.ds(0, groups - 1)], recv_two.at[1])
    second = {b: surface(landed_two[j]) for j, b in enumerate(blocks_of(1, groups))}
    for bit in (2, 4):
        second = butterfly(second, bit, lane)
    pieces = {b: partial[b // 2] for b in first} | second
    for bit in (8, 1):
        pieces = butterfly(pieces, bit, lane)
    for r in range(RADIX):
        s_out[pl.ds(TILE + r, own, stride=RADIX), :] = pieces[r]

    arrived(landed_ends.at[pl.ds(0, groups - 1)], recv_ends)
    edge = pltpu.roll(surface(landed_ends[:, 0, :]), 0, 1, stride=2 * TILE, stride_axis=0)
    lane = lax.broadcasted_iota(jnp.int32, (groups, LANES), 1)
    source = lax.broadcasted_iota(jnp.int32, (groups, LANES), 0)
    for at, r in ((-2, RADIX - 2), (-1, RADIX - 1), (count, 0), (count + 1, 1)):
        total_row = None
        for sub in range(2):
            shift = (sub - (r - sub * RADIX // 2)) * TILE % LANES
            moved = pltpu.roll(edge, shift, 1) if shift else edge
            moved = jnp.where(lane // TILE == 2 * source + sub, moved, 0.0)
            total_row = moved if sub == 0 else total_row + moved
        s_out[TILE + at : TILE + at + 1, :] = jnp.sum(total_row, axis=0, keepdims=True)

    for which in range(2):
        arrived(landed_sides.at[which], recv_side.at[which])
        sides[which] = surface(landed_sides[which])

    arrived(turned.at[pl.ds(0, (groups - 1) * ys)], send_one)
    arrived(product_one.at[pl.ds(0, groups - 1)], send_two)
    arrived(product_two.at[pl.ds(0, groups - 1)], send_two)
    arrived(ends.at[pl.ds(0, groups - 1)], send_ends)

    @pl.when(jnp.logical_or(gx == 0, gx == groups - 1))
    def _():
        arrived(side_parts, send_side)

    arrived(bests, recv_max)
    arrived(bests, send_max)
    peak = jnp.max(landed_ends[:, 1, :], axis=0, keepdims=True)
    for d in range(groups * (columns - 1)):
        peak = jnp.maximum(peak, bests[d])
    peak_out[...] = peak


def surface_by_kernel(coefficients, spacing, groups, columns):
    _, modes, ys = coefficients.shape
    full, twiddle = transform_tables()
    high = full.astype(jnp.bfloat16)
    low = (full - high.astype(np.float32)).astype(jnp.bfloat16)
    basis = np.concatenate([high, low], axis=0)
    weights = level_weights(spacing.shape[0])
    levels = spacing.shape[0] + 1
    count = NX // groups
    own = count // RADIX
    width = RADIX * TILE
    vmem = pl.BlockSpec(memory_space=pltpu.VMEM)
    hbm = pl.BlockSpec(memory_space=pltpu.HBM)
    dma = pltpu.SemaphoreType.DMA
    f32 = jnp.float32
    return pl.pallas_call(
        functools.partial(surface_kernel, groups, columns),
        out_shape=(
            pltpu.VMEM((count + 2 * TILE, ys), f32),
            pltpu.VMEM((2, TILE, LANES), f32),
            pltpu.VMEM((4, levels, LANES), f32),
            pltpu.VMEM((1, LANES), f32),
        ),
        in_specs=[hbm] * 5,
        out_specs=(vmem,) * 4,
        scratch_shapes=[
            pltpu.VMEM(coefficients.shape, f32),
            pltpu.VMEM((1, spacing.shape[0]), f32),
            pltpu.VMEM(weights.shape, f32),
            pltpu.VMEM(basis.shape, jnp.bfloat16),
            pltpu.VMEM(twiddle.shape, f32),
            pltpu.VMEM((ys, 2 * modes), f32),
            pltpu.VMEM((2, groups, TILE, 2 * modes), f32),
            pltpu.VMEM((2 * width, 2 * modes), jnp.bfloat16),
        ]
        + [pltpu.VMEM((groups, own, LANES), f32)] * 4
        + [
            pltpu.VMEM((groups, 2, LANES), f32),
            pltpu.VMEM((groups, 2, LANES), f32),
            pltpu.VMEM((groups, TILE, LANES), f32),
            pltpu.VMEM((2, TILE, LANES), f32),
            pltpu.VMEM((1, LANES), f32),
            pltpu.VMEM((groups * (columns - 1), 1, LANES), f32),
            pltpu.VMEM((groups, own, LANES), f32),
            dma((5,)),
            dma(()),
            dma((2,)),
            dma(()),
            dma((2,)),
            dma(()),
            dma(()),
            dma(()),
            dma((2,)),
            dma(()),
            dma(()),
            pltpu.SemaphoreType.REGULAR,
        ],
        compiler_params=pltpu.CompilerParams(
            collective_id=0, has_side_effects=True, vmem_limit_bytes=12 << 20
        ),
    )(*[
        pltpu.with_memory_space_constraint(jnp.asarray(x), pltpu.HBM)
        for x in (coefficients, spacing[None], weights, basis, twiddle)
    ])


def surface_by_gather(coefficients, spacing, groups):
    x_count = NX // groups
    x_first = lax.axis_index("gx") * x_count
    x_cells = x_first + jnp.arange(x_count, dtype=jnp.int32)
    portion = lax.all_gather(coefficients, "gx", axis=1, tiled=True)
    cosine, sine = basis(portion.shape[1], x_cells)
    surface = TOPO_SCALE * jnp.tanh(project(cosine, sine, portion) * 0.25)
    stretch = stretching(spacing)
    scale = stretch.shape[0] - 1.0
    slope = vertical(stretch)
    peak = lax.pmax(jnp.max(surface), ("gx", "gy"))
    wide = extended(surface, (("gx", 0), ("gy", 1)), 2)
    dx = (8.0 * (wide[3:-1] - wide[1:-3]) - (wide[4:] - wide[:-4]))[:, 2:-2] / 12.0
    dy = (8.0 * (wide[:, 3:-1] - wide[:, 1:-3]) - (wide[:, 4:] - wide[:, :-4]))[2:-2] / 12.0
    rows = [scale * stretch, scale * (1.0 - stretch), scale * slope]
    rows.append(slope / ((1.0 - peak) * jnp.min(slope)))
    table = jnp.broadcast_to(jnp.stack(rows)[:, :, None], (4, stretch.shape[0], LANES))
    return surface, dx, dy, table


def levels_kernel(depth, s_ref, dx_ref, dy_ref, table, z_ref, slopes_ref, jac_ref, quality_ref):
    first = pl.program_id(0) * depth

    def row(which, level):
        return table[which, pl.ds(first + level, 1), :]

    for level in range(depth):
        s, gain = s_ref[...], row(1, level)
        z_ref[level] = row(0, level) + gain * s
        slopes_ref[0, level] = gain * dx_ref[...]
        slopes_ref[1, level] = gain * dy_ref[...]
        rest = 1.0 - s
        jac_ref[level] = row(2, level) * rest
        quality_ref[level] = row(3, level) * rest


def all_levels(s, dx, dy, table):
    levels = table.shape[1]
    rows, columns = s.shape
    depth = 2
    plane = pl.BlockSpec((rows, columns), lambda i: (0, 0))
    field = pl.BlockSpec((depth, rows, columns), lambda i: (i, 0, 0))
    shape = jax.ShapeDtypeStruct((levels, rows, columns), jnp.float32)
    return pl.pallas_call(
        functools.partial(levels_kernel, depth),
        grid=(levels // depth,),
        in_specs=[plane, plane, plane, pl.BlockSpec(table.shape, lambda i: (0, 0, 0))],
        out_specs=(
            field,
            pl.BlockSpec((2, depth, rows, columns), lambda i: (0, i, 0, 0)),
            field,
            field,
        ),
        out_shape=(
            shape,
            jax.ShapeDtypeStruct((2, levels, rows, columns), jnp.float32),
            shape,
            shape,
        ),
    )(s, dx, dy, table)


def write_kernel(
    s_ref, sides, table, peak, z_hbm, slopes_hbm, jac_hbm, quality_hbm,
    z, slopes, jac, quality, dx, dy, outer, scaled, sems,
):
    levels, count, _ = z.shape
    own = count // RADIX
    inner = pl.ds(TILE, count)

    def row(which, level):
        return table[which, pl.ds(level, 1), :]

    def put(src, dst, at, which):
        pltpu.make_async_copy(src.at[at], dst.at[at], sems.at[which]).start()

    def heights(level, carry):
        s = s_ref[inner, :]
        z[level] = row(0, level) + row(1, level) * s
        put(z, z_hbm, level, 0)
        jac[level] = row(2, level) * (1.0 - s)
        put(jac, jac_hbm, level, 2)
        return carry

    lax.fori_loop(0, levels, heights, 0)
    highest = surface(jnp.max(peak[...], axis=1, keepdims=True))
    scaled[...] = table[3] / (1.0 - highest)

    def near(by):
        return s_ref[pl.ds(TILE + by, count), :]

    dx[...] = (8.0 * (near(1) - near(-1)) - (near(2) - near(-2))) * (1.0 / 12.0)
    lane = lax.broadcasted_iota(jnp.int32, (TILE, LANES), 1)
    for r in range(RADIX):
        for k in range(own // TILE):
            shift = LANES - r * TILE - 2 * k
            right = pltpu.roll(sides[0], shift % LANES, 1) if shift % LANES else sides[0]
            left = pltpu.roll(sides[1], (shift - 2) % LANES, 1) if (shift - 2) % LANES else sides[1]
            outer[pl.ds(k * TILE * RADIX + r, TILE, stride=RADIX), :] = jnp.where(
                lane < LANES // 2, right, left
            )
    s, edge = s_ref[inner, :], outer[...]
    lane = lax.broadcasted_iota(jnp.int32, (count, LANES), 1)

    def moved(by):
        taken = lane < by if by > 0 else lane >= LANES + by
        return pltpu.roll(jnp.where(taken, edge, s), (LANES - by) % LANES, 1)

    dy[...] = (8.0 * (moved(1) - moved(-1)) - (moved(2) - moved(-2))) * (1.0 / 12.0)

    def tilts(level, carry):
        gain = row(1, level)
        for at, slope in enumerate((dx, dy)):
            slopes[at, level] = gain * slope[...]
            put(slopes, slopes_hbm, (at, level), 1)
        quality[level] = scaled[pl.ds(level, 1), :] * (1.0 - s_ref[inner, :])
        put(quality, quality_hbm, level, 3)
        return carry

    lax.fori_loop(0, levels, tilts, 0)
    for i, (src, dst) in enumerate(
        ((z, z_hbm), (slopes, slopes_hbm), (jac, jac_hbm), (quality, quality_hbm))
    ):
        pltpu.make_async_copy(src, dst, sems.at[i]).wait()


def write_all(s, sides, table, peak):
    levels = table.shape[1]
    count, columns = s.shape[0] - 2 * TILE, s.shape[1]
    vmem = pl.BlockSpec(memory_space=pltpu.VMEM)
    hbm = pl.BlockSpec(memory_space=pl.ANY)
    field = (levels, count, columns)
    fields = (field, (2,) + field, field, field)
    f32 = jnp.float32
    plane = pltpu.VMEM((count, columns), f32)
    return pl.pallas_call(
        write_kernel,
        in_specs=[vmem] * 4,
        out_specs=(hbm,) * 4,
        out_shape=tuple(jax.ShapeDtypeStruct(shape, f32) for shape in fields),
        scratch_shapes=[pltpu.VMEM(shape, f32) for shape in fields]
        + [plane, plane, plane, pltpu.VMEM((levels, LANES), f32), pltpu.SemaphoreType.DMA((4,))],
        compiler_params=pltpu.CompilerParams(vmem_limit_bytes=48 << 20),
    )(s, sides, table, peak)


def shards(coefficients, spacing):
    groups, columns = lax.axis_size("gx"), lax.axis_size("gy")
    _, modes, ys = coefficients.shape
    fits = (
        groups == 8
        and ys == LANES
        and ys == groups * RADIX
        and modes == NX // RADIX
        and modes % LANES == 0
        and columns > 1
    )
    if fits:
        return write_all(*surface_by_kernel(coefficients, spacing, groups, columns))
    return all_levels(*surface_by_gather(coefficients, spacing, groups))


def solution(mesh):
    return jax.shard_map(
        shards,
        mesh=mesh,
        in_specs=(P(None, "gx", "gy"), P()),
        out_specs=(
            P(None, "gx", "gy"),
            P(None, None, "gx", "gy"),
            P(None, "gx", "gy"),
            P(None, "gx", "gy"),
        ),
        check_vma=False,
    )
```

```python
import functools
import math

import jax
import jax.numpy as jnp
import numpy as np
from jax import lax
from jax.experimental import pallas as pl
from jax.experimental.pallas import tpu as pltpu
from jax.sharding import PartitionSpec as P

NX = 4096


BOUNDARY = (
    (-24.0 / 17.0, 59.0 / 34.0, -4.0 / 17.0, -3.0 / 34.0, 0.0, 0.0),
    (-0.5, 0.0, 0.5, 0.0, 0.0, 0.0),
    (4.0 / 43.0, -59.0 / 86.0, 0.0, 59.0 / 86.0, -4.0 / 43.0, 0.0),
    (3.0 / 98.0, 0.0, -59.0 / 98.0, 0.0, 32.0 / 49.0, -4.0 / 49.0),
)
TOPO_SCALE = 0.1


def extended(cells, sides, width):
    for axis, dim in sides:
        count = lax.axis_size(axis)
        head = lax.slice_in_dim(cells, 0, width, axis=dim)
        tail = lax.slice_in_dim(cells, cells.shape[dim] - width, cells.shape[dim], axis=dim)
        cells = jnp.concatenate(
            [
                lax.ppermute(tail, axis, [(i, (i + 1) % count) for i in range(count)]),
                cells,
                lax.ppermute(head, axis, [((i + 1) % count, i) for i in range(count)]),
            ],
            axis=dim,
        )
    return cells


def vertical(field):
    levels = field.shape[0]
    top_rows = []
    bottom_rows = []
    for row_id in range(4):
        upper = None
        lower = None
        for level_id, factor in enumerate(BOUNDARY[row_id]):
            if factor != 0.0:
                term_up = factor * field[level_id]
                term_down = -factor * field[levels - 1 - level_id]
                upper = term_up if upper is None else upper + term_up
                lower = term_down if lower is None else lower + term_down
        top_rows.append(upper)
        bottom_rows.append(lower)
    inner = (
        8.0 * (field[5 : levels - 3] - field[3 : levels - 5])
        - (field[6 : levels - 2] - field[2 : levels - 6])
    ) / 12.0
    return jnp.concatenate([jnp.stack(top_rows), inner, jnp.stack(bottom_rows[::-1])], axis=0)


def stretching(spacing):
    summed = jnp.sum(spacing)
    return jnp.concatenate([jnp.zeros((1,), spacing.dtype), jnp.cumsum(spacing)]) / summed


def column_depth(surface, stretch):
    levels = stretch.shape[0]
    return (levels - 1.0) * (surface[None] + (1.0 - surface[None]) * stretch[:, None, None])


def basis(count, x_cells):
    mode_ids = jnp.arange(count, dtype=jnp.int32)
    phase = (mode_ids[:, None] * x_cells[None, :] % NX).astype(jnp.float32) * (2.0 * math.pi / NX)
    return (jnp.cos(phase), jnp.sin(phase))


def project(cosine, sine, portion):
    first = jnp.dot(
        cosine.T, portion[0], precision=lax.Precision.HIGHEST, preferred_element_type=jnp.float32
    )
    return first + jnp.dot(
        sine.T, portion[1], precision=lax.Precision.HIGHEST, preferred_element_type=jnp.float32
    )


LANES = 128
RADIX = 16
TILE = 8
MESH = pl.DeviceIdType.MESH


def level_weights(gaps):
    levels = gaps + 1
    summed = np.tril(np.ones((levels, gaps)), -1)
    deriv = np.zeros((levels, levels))
    for row in range(levels):
        if row < 4:
            deriv[row, :6] = BOUNDARY[row]
        elif row >= levels - 4:
            deriv[row, ::-1][:6] = -np.array(BOUNDARY[levels - 1 - row])
        else:
            deriv[row, row - 2 : row + 3] = np.array([1.0, -8.0, 0.0, 8.0, -1.0]) / 12.0
    return np.stack([summed, deriv @ summed]).astype(np.float32)


def transform_tables():
    part = NX // RADIX
    angle = 2.0 * np.pi / part * ((np.arange(part)[:, None] * np.arange(part)[None]) % part)
    full = np.concatenate([np.cos(angle), np.sin(angle)], axis=1).astype(np.float32)
    turn = 2.0 * np.pi / NX * (np.arange(RADIX)[:, None] * np.arange(part)[None])
    twiddle = np.concatenate([np.cos(turn), np.sin(turn)], axis=1).astype(np.float32)
    return full, twiddle


def rotate(value, angle):
    re, im = value
    cos, sin = math.cos(angle), math.sin(angle)
    if abs(sin) < 1e-12:
        return (re, im) if cos > 0 else (-re, -im)
    if abs(cos) < 1e-12:
        return (im, -re) if sin > 0 else (-im, re)
    if abs(abs(cos) - abs(sin)) < 1e-12:
        unit = math.sqrt(0.5)
        a, b = math.copysign(1.0, cos), math.copysign(1.0, sin)
        one = re * unit if a > 0 else re * -unit
        two = im * unit if a > 0 else im * -unit
        if a == b:
            return one + two, two - one
        return one - two, two + one
    return re * cos + im * sin, im * cos - re * sin


def fourier(values):
    count = len(values)
    if count == 1:
        return values
    even, odd = fourier(values[0::2]), fourier(values[1::2])
    out = [None] * count
    for i in range(count // 2):
        re, im = rotate(odd[i], 2.0 * math.pi * i / count)
        out[i] = (even[i][0] + re, even[i][1] + im)
        out[i + count // 2] = (even[i][0] - re, even[i][1] - im)
    return out


def split(value):
    high = value.astype(jnp.bfloat16)
    return high, (value - high.astype(jnp.float32)).astype(jnp.bfloat16)


def butterfly(values, bit, lane):
    shift = bit * TILE
    upper = (lane // TILE) & bit != 0
    for i in sorted(values):
        if not i & bit and i | bit in values:
            low, high = values[i], values[i | bit]
            values[i] = jnp.where(upper, pltpu.roll(high, shift, 1), low)
            values[i | bit] = jnp.where(upper, high, pltpu.roll(low, LANES - shift, 1))
    return values


def blocks_of(chunk, groups):
    return [2 * j + (chunk + j // (groups // 2)) % 2 for j in range(groups)]


def surface(raw):
    return TOPO_SCALE * jnp.tanh(raw * 0.25)


def arrived(view, sem):
    pltpu.make_async_copy(view, view, sem).wait()


def surface_kernel(
    groups, columns, coef_hbm, spacing_hbm, weights_hbm, basis_hbm, twiddle_hbm,
    s_out, sides, table, peak_out,
    coef, spacing, weights, basis, twiddle, turned, gathered, operand,
    product_one, product_two, landed_one, landed_two, ends, landed_ends,
    side_parts, landed_sides, best, bests, partial,
    load_sem, send_one, recv_one, send_two, recv_two, send_ends, recv_ends,
    send_side, recv_side, send_max, recv_max, later_sem,
):
    gx, gy = lax.axis_index("gx"), lax.axis_index("gy")
    cores, rows_of = 2, groups // 2

    def other(d):
        core = lax.rem(gx + d % cores, cores)
        row = lax.rem(gx // rows_of + d // rows_of, 2)
        col = lax.rem(gx // cores + (d // cores) % 2, 2)
        return row * rows_of + col * cores + core

    peers = [other(d) for d in (6, 7, 2, 3, 4, 5, 1)]
    loads = [
        pltpu.make_async_copy(src, dst, load_sem.at[i])
        for i, (src, dst) in enumerate((
            (coef_hbm, coef),
            (spacing_hbm, spacing),
            (weights_hbm, weights),
            (twiddle_hbm, twiddle),
            (basis_hbm, basis),
        ))
    ]
    loads[0].start()
    barrier = pltpu.get_barrier_semaphore()
    for peer in peers:
        pl.semaphore_signal(barrier, inc=1, device_id=(peer, gy), device_id_type=MESH)
    for up in range(1, columns):

        @pl.when(gy + up < columns)
        def _():
            for d in range(groups):
                target = (lax.rem(gx + d, groups), gy + up)
                pl.semaphore_signal(barrier, inc=1, device_id=target, device_id_type=MESH)

    part = coef.shape[1]
    ys = coef.shape[2] // groups
    half = NX // RADIX
    flip = gx // rows_of

    def sub_of(chunk, target):
        return lax.rem(chunk + target // rows_of, 2)

    def turned_rows(chunk, target):
        return pl.ds(pl.multiple_of(target * ys + sub_of(chunk, target) * TILE, TILE), TILE)

    loads[0].wait()
    for load in loads[1:]:
        load.start()
    turned[:, :part] = coef[0].T
    turned[:, part:] = coef[1].T
    pl.semaphore_wait(barrier, groups - 1 + groups * gy)

    far, close = peers[:2], peers[2:]
    order = [(chunk, peer) for some in (far, close) for chunk in range(2) for peer in some]
    for chunk, target in order:
        pltpu.make_async_remote_copy(
            src_ref=turned.at[turned_rows(chunk, target)],
            dst_ref=gathered.at[chunk, gx],
            send_sem=send_one,
            recv_sem=recv_one.at[chunk],
            device_id=(target, gy),
            device_id_type=MESH,
        ).start()
    for down in range(1, columns):

        @pl.when(gy >= down)
        def _():
            for d in range(groups):
                target = (lax.rem(gx + d, groups), gy - down)
                pl.semaphore_signal(later_sem, inc=1, device_id=target, device_id_type=MESH)

    for chunk in range(2):
        gathered[chunk, gx] = turned[turned_rows(chunk, gx), :]

    for load in loads[1:]:
        load.wait()
    thick = spacing[...]
    total = jnp.sum(thick, axis=1, keepdims=True)
    scale = spacing.shape[1] * 1.0
    levels = spacing.shape[1] + 1
    stretch = jnp.sum(weights[0] * thick, axis=1, keepdims=True) / total
    slope = jnp.sum(weights[1] * thick, axis=1, keepdims=True) / total
    least = jnp.min(slope, axis=0, keepdims=True)
    table[0] = jnp.broadcast_to(scale * stretch, (levels, LANES))
    table[1] = jnp.broadcast_to(scale * (1.0 - stretch), (levels, LANES))
    table[2] = jnp.broadcast_to(scale * slope, (levels, LANES))
    table[3] = jnp.broadcast_to(slope / least, (levels, LANES))

    rows = basis.shape[0] // 2
    own = rows // groups
    count = own * RADIX
    width = RADIX * TILE
    dot = functools.partial(
        lax.dot_general,
        dimension_numbers=(((1,), (1,)), ((), ())),
        preferred_element_type=jnp.float32,
    )

    def transform(chunk):
        values = [
            (gathered[chunk, i, :, :part], gathered[chunk, i, :, part:]) for i in range(groups)
        ]
        even = fourier(values)
        odd = fourier([rotate(v, 2.0 * math.pi * i / RADIX) for i, v in enumerate(values)])
        for r in range(0, RADIX, 2):
            pair = []
            for k, (re, im) in ((r, even[r // 2]), (r + 1, odd[r // 2])):
                if k:
                    cos, sin = twiddle[k : k + 1, :half], twiddle[k : k + 1, half:]
                    re, im = re * cos + im * sin, im * cos - re * sin
                pair.append((re, im))
            for at, lanes in enumerate((slice(0, half), slice(half, 2 * half))):
                high, low = split(jnp.concatenate([pair[0][at], pair[1][at]], axis=0))
                operand[r * TILE : (r + 2) * TILE, lanes] = high
                operand[width + r * TILE : width + (r + 2) * TILE, lanes] = low
        both = dot(basis[:rows], operand[...])
        return both[:, :width] + both[:, width:] + dot(basis[rows:], operand[:width])

    def send_product(chunk, some):
        product, landed = ((product_one, landed_one), (product_two, landed_two))[chunk]
        for target in some:
            pltpu.make_async_remote_copy(
                src_ref=product.at[target],
                dst_ref=landed.at[gx],
                send_sem=send_two,
                recv_sem=recv_two.at[chunk],
                device_id=(target, gy),
                device_id_type=MESH,
            ).start()

    def tallest(raw):
        return functools.reduce(jnp.maximum, [raw[i : i + TILE] for i in range(0, rows, TILE)])

    row_lane = lax.broadcasted_iota(jnp.int32, (1, LANES), 1)

    def ends_of(raw):
        return [
            jnp.where(
                row_lane < LANES // 2,
                raw[(dest + 1) * own % rows : (dest + 1) * own % rows + 1],
                raw[(dest * own - 1) % rows : (dest * own - 1) % rows + 1],
            )
            for dest in range(groups)
        ]

    def send_best(target, slot):
        for d in range(groups):
            pltpu.make_async_remote_copy(
                src_ref=best,
                dst_ref=bests.at[slot * groups + gx],
                send_sem=send_max,
                recv_sem=recv_max,
                device_id=(lax.rem(gx + d, groups), target),
                device_id_type=MESH,
            ).start()

    lane_one = lax.broadcasted_iota(jnp.int32, (TILE, LANES), 1)

    def pack_sides():
        for dest in range(groups):
            packed = None
            for k in range(own // TILE):
                shift = jnp.where(flip == 0, 2 * k, (2 * k + 2 - TILE) % LANES)
                tile = pltpu.roll(product_one[dest, k * TILE : (k + 1) * TILE], shift, 1)
                packed = tile if k == 0 else jnp.where(lane_one % TILE // 2 == k, tile, packed)
            side_parts[dest] = packed

    def send_sides(to_lower):
        for which, sender in enumerate((0, groups - 1)):
            column = lax.rem(gy + (columns - 1, 1)[which], columns)

            @pl.when(jnp.logical_and(gx == sender, (column < gy) if to_lower else (column > gy)))
            def _():
                for dest in range(groups):
                    pltpu.make_async_remote_copy(
                        src_ref=side_parts.at[dest],
                        dst_ref=landed_sides.at[which],
                        send_sem=send_side,
                        recv_sem=recv_side.at[which],
                        device_id=(dest, column),
                        device_id_type=MESH,
                    ).start()

    arrived(gathered.at[0, pl.ds(0, groups - 1)], recv_one.at[0])
    raw = transform(0)
    for dest in range(groups):
        product_one[dest] = raw[dest * own : (dest + 1) * own]
    @pl.when(gy < columns - 1)
    def _():
        send_product(0, far + close[2:])

    landed_one[gx] = product_one[gx]
    ends_one = ends_of(raw)
    peak_one = tallest(raw)

    arrived(gathered.at[1, pl.ds(0, groups - 1)], recv_one.at[1])
    raw = transform(1)
    for dest in range(groups):
        product_two[dest] = raw[dest * own : (dest + 1) * own]
    pack_sides()
    best[...] = jnp.max(jnp.maximum(peak_one, tallest(raw)), axis=0, keepdims=True)
    for down in range(columns - 1, 0, -1):

        @pl.when(gy >= down)
        def _():
            send_best(gy - down, down - 1)

        if down == columns - 1:
            send_sides(True)

    @pl.when(gy == columns - 1)
    def _():
        send_product(0, far)
        send_product(1, far)
        send_product(0, close)

    @pl.when(gy < columns - 1)
    def _():
        send_product(1, far)
        send_product(0, close[:2])

    send_product(1, close[2:] + close[:2])
    landed_two[gx] = product_two[gx]
    ends_two = ends_of(raw)
    outside = jnp.abs(row_lane // TILE * 2 - (RADIX - 1)) > RADIX // 2
    for dest in range(groups):
        one, two = ends_one[dest], ends_two[dest]
        low, high = jnp.where(flip == 0, one, two), jnp.where(flip == 0, two, one)
        ends[dest, 0:1] = jnp.where(outside, low, pltpu.roll(high, LANES // 2, 1))
        ends[dest, 1:2] = best[...]
    for target in peers:
        pltpu.make_async_remote_copy(
            src_ref=ends.at[target],
            dst_ref=landed_ends.at[gx],
            send_sem=send_ends,
            recv_sem=recv_ends,
            device_id=(target, gy),
            device_id_type=MESH,
        ).start()
    landed_ends[gx] = ends[gx]

    @pl.when(gy < columns - 1)
    def _():
        pl.semaphore_wait(later_sem, groups * (columns - 1 - gy))

    send_sides(False)

    for up in range(1, columns):

        @pl.when(gy + up < columns)
        def _():
            send_best(gy + up, columns - up - 1)

    lane = lax.broadcasted_iota(jnp.int32, (own, LANES), 1)
    arrived(landed_one.at[pl.ds(0, groups - 1)], recv_two.at[0])
    first = {b: surface(landed_one[j]) for j, b in enumerate(blocks_of(0, groups))}
    for bit in (2, 4):
        first = butterfly(first, bit, lane)
    for b, value in first.items():
        partial[b // 2] = value

    arrived(landed_two.at[pl.ds(0, groups - 1)], recv_two.at[1])
    second = {b: surface(landed_two[j]) for j, b in enumerate(blocks_of(1, groups))}
    for bit in (2, 4):
        second = butterfly(second, bit, lane)
    pieces = {b: partial[b // 2] for b in first} | second
    for bit in (8, 1):
        pieces = butterfly(pieces, bit, lane)
    for r in range(RADIX):
        s_out[pl.ds(TILE + r, own, stride=RADIX), :] = pieces[r]

    arrived(landed_ends.at[pl.ds(0, groups - 1)], recv_ends)
    edge = pltpu.roll(surface(landed_ends[:, 0, :]), 0, 1, stride=2 * TILE, stride_axis=0)
    lane = lax.broadcasted_iota(jnp.int32, (groups, LANES), 1)
    source = lax.broadcasted_iota(jnp.int32, (groups, LANES), 0)
    for at, r in ((-2, RADIX - 2), (-1, RADIX - 1), (count, 0), (count + 1, 1)):
        total_row = None
        for sub in range(2):
            shift = (sub - (r - sub * RADIX // 2)) * TILE % LANES
            moved = pltpu.roll(edge, shift, 1) if shift else edge
            moved = jnp.where(lane // TILE == 2 * source + sub, moved, 0.0)
            total_row = moved if sub == 0 else total_row + moved
        s_out[TILE + at : TILE + at + 1, :] = jnp.sum(total_row, axis=0, keepdims=True)

    for which in range(2):
        arrived(landed_sides.at[which], recv_side.at[which])
        sides[which] = surface(landed_sides[which])

    arrived(turned.at[pl.ds(0, (groups - 1) * ys)], send_one)
    arrived(product_one.at[pl.ds(0, groups - 1)], send_two)
    arrived(product_two.at[pl.ds(0, groups - 1)], send_two)
    arrived(ends.at[pl.ds(0, groups - 1)], send_ends)

    @pl.when(jnp.logical_or(gx == 0, gx == groups - 1))
    def _():
        arrived(side_parts, send_side)

    arrived(bests, recv_max)
    arrived(bests, send_max)
    peak = jnp.max(landed_ends[:, 1, :], axis=0, keepdims=True)
    for d in range(groups * (columns - 1)):
        peak = jnp.maximum(peak, bests[d])
    peak_out[...] = peak


def surface_by_kernel(coefficients, spacing, groups, columns):
    _, modes, ys = coefficients.shape
    full, twiddle = transform_tables()
    high = full.astype(jnp.bfloat16)
    low = (full - high.astype(np.float32)).astype(jnp.bfloat16)
    basis = np.concatenate([high, low], axis=0)
    weights = level_weights(spacing.shape[0])
    levels = spacing.shape[0] + 1
    count = NX // groups
    own = count // RADIX
    width = RADIX * TILE
    vmem = pl.BlockSpec(memory_space=pltpu.VMEM)
    hbm = pl.BlockSpec(memory_space=pltpu.HBM)
    dma = pltpu.SemaphoreType.DMA
    f32 = jnp.float32
    return pl.pallas_call(
        functools.partial(surface_kernel, groups, columns),
        out_shape=(
            pltpu.VMEM((count + 2 * TILE, ys), f32),
            pltpu.VMEM((2, TILE, LANES), f32),
            pltpu.VMEM((4, levels, LANES), f32),
            pltpu.VMEM((1, LANES), f32),
        ),
        in_specs=[hbm] * 5,
        out_specs=(vmem,) * 4,
        scratch_shapes=[
            pltpu.VMEM(coefficients.shape, f32),
            pltpu.VMEM((1, spacing.shape[0]), f32),
            pltpu.VMEM(weights.shape, f32),
            pltpu.VMEM(basis.shape, jnp.bfloat16),
            pltpu.VMEM(twiddle.shape, f32),
            pltpu.VMEM((ys, 2 * modes), f32),
            pltpu.VMEM((2, groups, TILE, 2 * modes), f32),
            pltpu.VMEM((2 * width, 2 * modes), jnp.bfloat16),
        ]
        + [pltpu.VMEM((groups, own, LANES), f32)] * 4
        + [
            pltpu.VMEM((groups, 2, LANES), f32),
            pltpu.VMEM((groups, 2, LANES), f32),
            pltpu.VMEM((groups, TILE, LANES), f32),
            pltpu.VMEM((2, TILE, LANES), f32),
            pltpu.VMEM((1, LANES), f32),
            pltpu.VMEM((groups * (columns - 1), 1, LANES), f32),
            pltpu.VMEM((groups, own, LANES), f32),
            dma((5,)),
            dma(()),
            dma((2,)),
            dma(()),
            dma((2,)),
            dma(()),
            dma(()),
            dma(()),
            dma((2,)),
            dma(()),
            dma(()),
            pltpu.SemaphoreType.REGULAR,
        ],
        compiler_params=pltpu.CompilerParams(
            collective_id=0, has_side_effects=True, vmem_limit_bytes=12 << 20
        ),
    )(*[
        pltpu.with_memory_space_constraint(jnp.asarray(x), pltpu.HBM)
        for x in (coefficients, spacing[None], weights, basis, twiddle)
    ])


def surface_by_gather(coefficients, spacing, groups):
    x_count = NX // groups
    x_first = lax.axis_index("gx") * x_count
    x_cells = x_first + jnp.arange(x_count, dtype=jnp.int32)
    portion = lax.all_gather(coefficients, "gx", axis=1, tiled=True)
    cosine, sine = basis(portion.shape[1], x_cells)
    surface = TOPO_SCALE * jnp.tanh(project(cosine, sine, portion) * 0.25)
    stretch = stretching(spacing)
    scale = stretch.shape[0] - 1.0
    slope = vertical(stretch)
    peak = lax.pmax(jnp.max(surface), ("gx", "gy"))
    wide = extended(surface, (("gx", 0), ("gy", 1)), 2)
    dx = (8.0 * (wide[3:-1] - wide[1:-3]) - (wide[4:] - wide[:-4]))[:, 2:-2] / 12.0
    dy = (8.0 * (wide[:, 3:-1] - wide[:, 1:-3]) - (wide[:, 4:] - wide[:, :-4]))[2:-2] / 12.0
    rows = [scale * stretch, scale * (1.0 - stretch), scale * slope]
    rows.append(slope / ((1.0 - peak) * jnp.min(slope)))
    table = jnp.broadcast_to(jnp.stack(rows)[:, :, None], (4, stretch.shape[0], LANES))
    return surface, dx, dy, table


def levels_kernel(depth, s_ref, dx_ref, dy_ref, table, z_ref, slopes_ref, jac_ref, quality_ref):
    first = pl.program_id(0) * depth

    def row(which, level):
        return table[which, pl.ds(first + level, 1), :]

    for level in range(depth):
        s, gain = s_ref[...], row(1, level)
        z_ref[level] = row(0, level) + gain * s
        slopes_ref[0, level] = gain * dx_ref[...]
        slopes_ref[1, level] = gain * dy_ref[...]
        rest = 1.0 - s
        jac_ref[level] = row(2, level) * rest
        quality_ref[level] = row(3, level) * rest


def all_levels(s, dx, dy, table):
    levels = table.shape[1]
    rows, columns = s.shape
    depth = 2
    plane = pl.BlockSpec((rows, columns), lambda i: (0, 0))
    field = pl.BlockSpec((depth, rows, columns), lambda i: (i, 0, 0))
    shape = jax.ShapeDtypeStruct((levels, rows, columns), jnp.float32)
    return pl.pallas_call(
        functools.partial(levels_kernel, depth),
        grid=(levels // depth,),
        in_specs=[plane, plane, plane, pl.BlockSpec(table.shape, lambda i: (0, 0, 0))],
        out_specs=(
            field,
            pl.BlockSpec((2, depth, rows, columns), lambda i: (0, i, 0, 0)),
            field,
            field,
        ),
        out_shape=(
            shape,
            jax.ShapeDtypeStruct((2, levels, rows, columns), jnp.float32),
            shape,
            shape,
        ),
    )(s, dx, dy, table)


def write_kernel(
    s_ref, sides, table, peak, z_hbm, slopes_hbm, jac_hbm, quality_hbm,
    z, slopes, jac, quality, dx, dy, outer, scaled, sems,
):
    levels, count, _ = z.shape
    own = count // RADIX
    inner = pl.ds(TILE, count)

    def row(which, level):
        return table[which, pl.ds(level, 1), :]

    def put(src, dst, at, which):
        pltpu.make_async_copy(src.at[at], dst.at[at], sems.at[which]).start()

    def heights(level, carry):
        s = s_ref[inner, :]
        z[level] = row(0, level) + row(1, level) * s
        put(z, z_hbm, level, 0)
        jac[level] = row(2, level) * (1.0 - s)
        put(jac, jac_hbm, level, 2)
        return carry

    lax.fori_loop(0, levels, heights, 0)
    highest = surface(jnp.max(peak[...], axis=1, keepdims=True))
    scaled[...] = table[3] / (1.0 - highest)

    def near(by):
        return s_ref[pl.ds(TILE + by, count), :]

    dx[...] = (8.0 * (near(1) - near(-1)) - (near(2) - near(-2))) * (1.0 / 12.0)
    lane = lax.broadcasted_iota(jnp.int32, (TILE, LANES), 1)
    for r in range(RADIX):
        for k in range(own // TILE):
            shift = LANES - r * TILE - 2 * k
            right = pltpu.roll(sides[0], shift % LANES, 1) if shift % LANES else sides[0]
            left = pltpu.roll(sides[1], (shift - 2) % LANES, 1) if (shift - 2) % LANES else sides[1]
            outer[pl.ds(k * TILE * RADIX + r, TILE, stride=RADIX), :] = jnp.where(
                lane < LANES // 2, right, left
            )
    s, edge = s_ref[inner, :], outer[...]
    lane = lax.broadcasted_iota(jnp.int32, (count, LANES), 1)

    def moved(by):
        taken = lane < by if by > 0 else lane >= LANES + by
        return pltpu.roll(jnp.where(taken, edge, s), (LANES - by) % LANES, 1)

    dy[...] = (8.0 * (moved(1) - moved(-1)) - (moved(2) - moved(-2))) * (1.0 / 12.0)

    def tilts(level, carry):
        gain = row(1, level)
        for at, slope in enumerate((dx, dy)):
            slopes[at, level] = gain * slope[...]
            put(slopes, slopes_hbm, (at, level), 1)
        quality[level] = scaled[pl.ds(level, 1), :] * (1.0 - s_ref[inner, :])
        put(quality, quality_hbm, level, 3)
        return carry

    lax.fori_loop(0, levels, tilts, 0)
    for i, (src, dst) in enumerate(
        ((z, z_hbm), (slopes, slopes_hbm), (jac, jac_hbm), (quality, quality_hbm))
    ):
        pltpu.make_async_copy(src, dst, sems.at[i]).wait()


def write_all(s, sides, table, peak):
    levels = table.shape[1]
    count, columns = s.shape[0] - 2 * TILE, s.shape[1]
    vmem = pl.BlockSpec(memory_space=pltpu.VMEM)
    hbm = pl.BlockSpec(memory_space=pl.ANY)
    field = (levels, count, columns)
    fields = (field, (2,) + field, field, field)
    f32 = jnp.float32
    plane = pltpu.VMEM((count, columns), f32)
    return pl.pallas_call(
        write_kernel,
        in_specs=[vmem] * 4,
        out_specs=(hbm,) * 4,
        out_shape=tuple(jax.ShapeDtypeStruct(shape, f32) for shape in fields),
        scratch_shapes=[pltpu.VMEM(shape, f32) for shape in fields]
        + [plane, plane, plane, pltpu.VMEM((levels, LANES), f32), pltpu.SemaphoreType.DMA((4,))],
        compiler_params=pltpu.CompilerParams(vmem_limit_bytes=48 << 20),
    )(s, sides, table, peak)


def shards(coefficients, spacing):
    groups, columns = lax.axis_size("gx"), lax.axis_size("gy")
    _, modes, ys = coefficients.shape
    fits = (
        groups == 8
        and ys == LANES
        and ys == groups * RADIX
        and modes == NX // RADIX
        and modes % LANES == 0
        and columns > 1
    )
    if fits:
        return write_all(*surface_by_kernel(coefficients, spacing, groups, columns))
    return all_levels(*surface_by_gather(coefficients, spacing, groups))


def solution(mesh):
    return jax.shard_map(
        shards,
        mesh=mesh,
        in_specs=(P(None, "gx", "gy"), P()),
        out_specs=(
            P(None, "gx", "gy"),
            P(None, None, "gx", "gy"),
            P(None, "gx", "gy"),
            P(None, "gx", "gy"),
        ),
        check_vma=False,
    )
```

```python
import functools
import math

import jax
import jax.numpy as jnp
import numpy as np
from jax import lax
from jax.experimental import pallas as pl
from jax.experimental.pallas import tpu as pltpu
from jax.sharding import PartitionSpec as P

NX = 4096


BOUNDARY = (
    (-24.0 / 17.0, 59.0 / 34.0, -4.0 / 17.0, -3.0 / 34.0, 0.0, 0.0),
    (-0.5, 0.0, 0.5, 0.0, 0.0, 0.0),
    (4.0 / 43.0, -59.0 / 86.0, 0.0, 59.0 / 86.0, -4.0 / 43.0, 0.0),
    (3.0 / 98.0, 0.0, -59.0 / 98.0, 0.0, 32.0 / 49.0, -4.0 / 49.0),
)
TOPO_SCALE = 0.1


def extended(cells, sides, width):
    for axis, dim in sides:
        count = lax.axis_size(axis)
        head = lax.slice_in_dim(cells, 0, width, axis=dim)
        tail = lax.slice_in_dim(cells, cells.shape[dim] - width, cells.shape[dim], axis=dim)
        cells = jnp.concatenate(
            [
                lax.ppermute(tail, axis, [(i, (i + 1) % count) for i in range(count)]),
                cells,
                lax.ppermute(head, axis, [((i + 1) % count, i) for i in range(count)]),
            ],
            axis=dim,
        )
    return cells


def vertical(field):
    levels = field.shape[0]
    top_rows = []
    bottom_rows = []
    for row_id in range(4):
        upper = None
        lower = None
        for level_id, factor in enumerate(BOUNDARY[row_id]):
            if factor != 0.0:
                term_up = factor * field[level_id]
                term_down = -factor * field[levels - 1 - level_id]
                upper = term_up if upper is None else upper + term_up
                lower = term_down if lower is None else lower + term_down
        top_rows.append(upper)
        bottom_rows.append(lower)
    inner = (
        8.0 * (field[5 : levels - 3] - field[3 : levels - 5])
        - (field[6 : levels - 2] - field[2 : levels - 6])
    ) / 12.0
    return jnp.concatenate([jnp.stack(top_rows), inner, jnp.stack(bottom_rows[::-1])], axis=0)


def stretching(spacing):
    summed = jnp.sum(spacing)
    return jnp.concatenate([jnp.zeros((1,), spacing.dtype), jnp.cumsum(spacing)]) / summed


def column_depth(surface, stretch):
    levels = stretch.shape[0]
    return (levels - 1.0) * (surface[None] + (1.0 - surface[None]) * stretch[:, None, None])


def basis(count, x_cells):
    mode_ids = jnp.arange(count, dtype=jnp.int32)
    phase = (mode_ids[:, None] * x_cells[None, :] % NX).astype(jnp.float32) * (2.0 * math.pi / NX)
    return (jnp.cos(phase), jnp.sin(phase))


def project(cosine, sine, portion):
    first = jnp.dot(
        cosine.T, portion[0], precision=lax.Precision.HIGHEST, preferred_element_type=jnp.float32
    )
    return first + jnp.dot(
        sine.T, portion[1], precision=lax.Precision.HIGHEST, preferred_element_type=jnp.float32
    )


LANES = 128
RADIX = 16
TILE = 8
MESH = pl.DeviceIdType.MESH


def level_weights(gaps):
    levels = gaps + 1
    summed = np.tril(np.ones((levels, gaps)), -1)
    deriv = np.zeros((levels, levels))
    for row in range(levels):
        if row < 4:
            deriv[row, :6] = BOUNDARY[row]
        elif row >= levels - 4:
            deriv[row, ::-1][:6] = -np.array(BOUNDARY[levels - 1 - row])
        else:
            deriv[row, row - 2 : row + 3] = np.array([1.0, -8.0, 0.0, 8.0, -1.0]) / 12.0
    return np.stack([summed, deriv @ summed]).astype(np.float32)


def transform_tables():
    part = NX // RADIX
    angle = 2.0 * np.pi / part * ((np.arange(part)[:, None] * np.arange(part)[None]) % part)
    full = np.concatenate([np.cos(angle), np.sin(angle)], axis=1).astype(np.float32)
    turn = 2.0 * np.pi / NX * (np.arange(RADIX)[:, None] * np.arange(part)[None])
    twiddle = np.concatenate([np.cos(turn), np.sin(turn)], axis=1).astype(np.float32)
    return full, twiddle


def rotate(value, angle):
    re, im = value
    cos, sin = math.cos(angle), math.sin(angle)
    if abs(sin) < 1e-12:
        return (re, im) if cos > 0 else (-re, -im)
    if abs(cos) < 1e-12:
        return (im, -re) if sin > 0 else (-im, re)
    if abs(abs(cos) - abs(sin)) < 1e-12:
        unit = math.sqrt(0.5)
        a, b = math.copysign(1.0, cos), math.copysign(1.0, sin)
        one = re * unit if a > 0 else re * -unit
        two = im * unit if a > 0 else im * -unit
        if a == b:
            return one + two, two - one
        return one - two, two + one
    return re * cos + im * sin, im * cos - re * sin


def fourier(values):
    count = len(values)
    if count == 1:
        return values
    even, odd = fourier(values[0::2]), fourier(values[1::2])
    out = [None] * count
    for i in range(count // 2):
        re, im = rotate(odd[i], 2.0 * math.pi * i / count)
        out[i] = (even[i][0] + re, even[i][1] + im)
        out[i + count // 2] = (even[i][0] - re, even[i][1] - im)
    return out


def split(value):
    high = value.astype(jnp.bfloat16)
    return high, (value - high.astype(jnp.float32)).astype(jnp.bfloat16)


def butterfly(values, bit, lane):
    shift = bit * TILE
    upper = (lane // TILE) & bit != 0
    for i in sorted(values):
        if not i & bit and i | bit in values:
            low, high = values[i], values[i | bit]
            values[i] = jnp.where(upper, pltpu.roll(high, shift, 1), low)
            values[i | bit] = jnp.where(upper, high, pltpu.roll(low, LANES - shift, 1))
    return values


def blocks_of(chunk, groups):
    return [2 * j + (chunk + j // (groups // 2)) % 2 for j in range(groups)]


def surface(raw):
    return TOPO_SCALE * jnp.tanh(raw * 0.25)


def arrived(view, sem):
    pltpu.make_async_copy(view, view, sem).wait()


def surface_kernel(
    groups, columns, coef_hbm, spacing_hbm, weights_hbm, basis_hbm, twiddle_hbm,
    s_out, sides, table, peak_out,
    coef, spacing, weights, basis, twiddle, turned, gathered, operand,
    product_one, product_two, landed_one, landed_two, ends, landed_ends,
    side_parts, landed_sides, best, bests, partial,
    load_sem, send_one, recv_one, send_two, recv_two, send_ends, recv_ends,
    send_side, recv_side, send_max, recv_max, later_sem,
):
    gx, gy = lax.axis_index("gx"), lax.axis_index("gy")
    cores, rows_of = 2, groups // 2
    flip = gx // rows_of
    col, core = gx // cores - flip * (rows_of // cores), gx - gx // cores * cores

    def other(d):
        places = (flip, d // rows_of), (col, d // cores % 2), (core, d % cores)
        row_to, col_to, core_to = [1 - at if moves else at for at, moves in places]
        return row_to * rows_of + col_to * cores + core_to

    peers = [other(d) for d in (6, 7, 2, 3, 4, 5, 1)]
    loads = [
        pltpu.make_async_copy(src, dst, load_sem.at[i])
        for i, (src, dst) in enumerate((
            (coef_hbm, coef),
            (spacing_hbm, spacing),
            (weights_hbm, weights),
            (twiddle_hbm, twiddle),
            (basis_hbm, basis),
        ))
    ]
    loads[0].start()
    barrier = pltpu.get_barrier_semaphore()
    for peer in peers:
        pl.semaphore_signal(barrier, inc=1, device_id=(peer, gy), device_id_type=MESH)
    for up in range(1, columns):

        @pl.when(gy + up < columns)
        def _():
            for d in range(groups):
                target = (lax.rem(gx + d, groups), gy + up)
                pl.semaphore_signal(barrier, inc=1, device_id=target, device_id_type=MESH)

    part = coef.shape[1]
    ys = coef.shape[2] // groups
    half = NX // RADIX

    def sub_of(chunk, target):
        return lax.rem(chunk + target // rows_of, 2)

    def turned_rows(chunk, target):
        return pl.ds(pl.multiple_of(target * ys + sub_of(chunk, target) * TILE, TILE), TILE)

    loads[0].wait()
    for load in loads[1:]:
        load.start()
    turned[:, :part] = coef[0].T
    turned[:, part:] = coef[1].T
    pl.semaphore_wait(barrier, groups - 1 + groups * gy)

    far, close = peers[:2], peers[2:]
    order = [(chunk, peer) for some in (far, close) for chunk in range(2) for peer in some]
    for chunk, target in order:
        pltpu.make_async_remote_copy(
            src_ref=turned.at[turned_rows(chunk, target)],
            dst_ref=gathered.at[chunk, gx],
            send_sem=send_one,
            recv_sem=recv_one.at[chunk],
            device_id=(target, gy),
            device_id_type=MESH,
        ).start()
    for down in range(1, columns):

        @pl.when(gy >= down)
        def _():
            for d in range(groups):
                target = (lax.rem(gx + d, groups), gy - down)
                pl.semaphore_signal(later_sem, inc=1, device_id=target, device_id_type=MESH)

    for chunk in range(2):
        gathered[chunk, gx] = turned[turned_rows(chunk, gx), :]

    for load in loads[1:]:
        load.wait()
    thick = spacing[...]
    total = jnp.sum(thick, axis=1, keepdims=True)
    scale = spacing.shape[1] * 1.0
    levels = spacing.shape[1] + 1
    stretch = jnp.sum(weights[0] * thick, axis=1, keepdims=True) / total
    slope = jnp.sum(weights[1] * thick, axis=1, keepdims=True) / total
    least = jnp.min(slope, axis=0, keepdims=True)
    table[0] = jnp.broadcast_to(scale * stretch, (levels, LANES))
    table[1] = jnp.broadcast_to(scale * (1.0 - stretch), (levels, LANES))
    table[2] = jnp.broadcast_to(scale * slope, (levels, LANES))
    table[3] = jnp.broadcast_to(slope / least, (levels, LANES))

    rows = basis.shape[0] // 2
    own = rows // groups
    count = own * RADIX
    width = RADIX * TILE
    dot = functools.partial(
        lax.dot_general,
        dimension_numbers=(((1,), (1,)), ((), ())),
        preferred_element_type=jnp.float32,
    )

    def transform(chunk):
        values = [
            (gathered[chunk, i, :, :part], gathered[chunk, i, :, part:]) for i in range(groups)
        ]
        even = fourier(values)
        odd = fourier([rotate(v, 2.0 * math.pi * i / RADIX) for i, v in enumerate(values)])
        for r in range(0, RADIX, 2):
            pair = []
            for k, (re, im) in ((r, even[r // 2]), (r + 1, odd[r // 2])):
                if k:
                    cos, sin = twiddle[k : k + 1, :half], twiddle[k : k + 1, half:]
                    re, im = re * cos + im * sin, im * cos - re * sin
                pair.append((re, im))
            for at, lanes in enumerate((slice(0, half), slice(half, 2 * half))):
                high, low = split(jnp.concatenate([pair[0][at], pair[1][at]], axis=0))
                operand[r * TILE : (r + 2) * TILE, lanes] = high
                operand[width + r * TILE : width + (r + 2) * TILE, lanes] = low
        small = dot(basis[rows:], operand[:width])
        both = dot(basis[:rows], operand[...])
        return both[:, :width] + (both[:, width:] + small)

    def send_product(product, landed, chunk):
        for target in peers:
            pltpu.make_async_remote_copy(
                src_ref=product.at[target],
                dst_ref=landed.at[gx],
                send_sem=send_two,
                recv_sem=recv_two.at[chunk],
                device_id=(target, gy),
                device_id_type=MESH,
            ).start()
        landed[gx] = product[gx]

    def tallest(raw):
        return functools.reduce(jnp.maximum, [raw[i : i + TILE] for i in range(0, rows, TILE)])

    row_lane = lax.broadcasted_iota(jnp.int32, (1, LANES), 1)

    def ends_of(raw):
        return [
            jnp.where(
                row_lane < LANES // 2,
                raw[(dest + 1) * own % rows : (dest + 1) * own % rows + 1],
                raw[(dest * own - 1) % rows : (dest * own - 1) % rows + 1],
            )
            for dest in range(groups)
        ]

    def send_best(target, slot):
        for d in range(groups):
            pltpu.make_async_remote_copy(
                src_ref=best,
                dst_ref=bests.at[slot * groups + gx],
                send_sem=send_max,
                recv_sem=recv_max,
                device_id=(lax.rem(gx + d, groups), target),
                device_id_type=MESH,
            ).start()

    lane_one = lax.broadcasted_iota(jnp.int32, (TILE, LANES), 1)

    def pack_sides():
        for dest in range(groups):
            packed = None
            for k in range(own // TILE):
                shift = jnp.where(flip == 0, 2 * k, (2 * k + 2 - TILE) % LANES)
                tile = pltpu.roll(product_one[dest, k * TILE : (k + 1) * TILE], shift, 1)
                packed = tile if k == 0 else jnp.where(lane_one % TILE // 2 == k, tile, packed)
            side_parts[dest] = packed

    def send_sides(to_lower):
        for which, sender in enumerate((0, groups - 1)):
            column = lax.rem(gy + (columns - 1, 1)[which], columns)

            @pl.when(jnp.logical_and(gx == sender, (column < gy) if to_lower else (column > gy)))
            def _():
                for dest in range(groups):
                    pltpu.make_async_remote_copy(
                        src_ref=side_parts.at[dest],
                        dst_ref=landed_sides.at[which],
                        send_sem=send_side,
                        recv_sem=recv_side.at[which],
                        device_id=(dest, column),
                        device_id_type=MESH,
                    ).start()

    arrived(gathered.at[0, pl.ds(0, groups - 1)], recv_one.at[0])
    raw = transform(0)
    for dest in range(groups):
        product_one[dest] = raw[dest * own : (dest + 1) * own]
    send_product(product_one, landed_one, 0)
    ends_one = ends_of(raw)
    peak_one = tallest(raw)

    arrived(gathered.at[1, pl.ds(0, groups - 1)], recv_one.at[1])
    raw = transform(1)
    for dest in range(groups):
        product_two[dest] = raw[dest * own : (dest + 1) * own]
    best[...] = jnp.max(jnp.maximum(peak_one, tallest(raw)), axis=0, keepdims=True)
    for down in range(columns - 1, 0, -1):

        @pl.when(gy >= down)
        def _():
            send_best(gy - down, down - 1)

        if down == columns - 1:
            pack_sides()
            send_sides(True)

    send_product(product_two, landed_two, 1)
    ends_two = ends_of(raw)
    outside = jnp.abs(row_lane // TILE * 2 - (RADIX - 1)) > RADIX // 2
    for dest in range(groups):
        one, two = ends_one[dest], ends_two[dest]
        low, high = jnp.where(flip == 0, one, two), jnp.where(flip == 0, two, one)
        ends[dest, 0:1] = jnp.where(outside, low, pltpu.roll(high, LANES // 2, 1))
        ends[dest, 1:2] = best[...]
    for target in peers:
        pltpu.make_async_remote_copy(
            src_ref=ends.at[target],
            dst_ref=landed_ends.at[gx],
            send_sem=send_ends,
            recv_sem=recv_ends,
            device_id=(target, gy),
            device_id_type=MESH,
        ).start()
    landed_ends[gx] = ends[gx]

    @pl.when(gy < columns - 1)
    def _():
        pl.semaphore_wait(later_sem, groups * (columns - 1 - gy))

    send_sides(False)

    for up in range(1, columns):

        @pl.when(gy + up < columns)
        def _():
            send_best(gy + up, columns - up - 1)

    lane = lax.broadcasted_iota(jnp.int32, (own, LANES), 1)
    arrived(landed_one.at[pl.ds(0, groups - 1)], recv_two.at[0])
    first = {b: surface(landed_one[j]) for j, b in enumerate(blocks_of(0, groups))}
    for bit in (2, 4):
        first = butterfly(first, bit, lane)
    for b, value in first.items():
        partial[b // 2] = value

    arrived(landed_two.at[pl.ds(0, groups - 1)], recv_two.at[1])
    second = {b: surface(landed_two[j]) for j, b in enumerate(blocks_of(1, groups))}
    for bit in (2, 4):
        second = butterfly(second, bit, lane)
    pieces = {b: partial[b // 2] for b in first} | second
    for bit in (8, 1):
        pieces = butterfly(pieces, bit, lane)
    for r in range(RADIX):
        s_out[pl.ds(TILE + r, own, stride=RADIX), :] = pieces[r]

    arrived(landed_ends.at[pl.ds(0, groups - 1)], recv_ends)
    edge = pltpu.roll(surface(landed_ends[:, 0, :]), 0, 1, stride=2 * TILE, stride_axis=0)
    lane = lax.broadcasted_iota(jnp.int32, (groups, LANES), 1)
    source = lax.broadcasted_iota(jnp.int32, (groups, LANES), 0)
    for at, r in ((-2, RADIX - 2), (-1, RADIX - 1), (count, 0), (count + 1, 1)):
        total_row = None
        for sub in range(2):
            shift = (sub - (r - sub * RADIX // 2)) * TILE % LANES
            moved = pltpu.roll(edge, shift, 1) if shift else edge
            moved = jnp.where(lane // TILE == 2 * source + sub, moved, 0.0)
            total_row = moved if sub == 0 else total_row + moved
        s_out[TILE + at : TILE + at + 1, :] = jnp.sum(total_row, axis=0, keepdims=True)

    for which in range(2):
        arrived(landed_sides.at[which], recv_side.at[which])
        sides[which] = surface(landed_sides[which])

    arrived(turned.at[pl.ds(0, (groups - 1) * ys)], send_one)
    arrived(product_one.at[pl.ds(0, groups - 1)], send_two)
    arrived(product_two.at[pl.ds(0, groups - 1)], send_two)
    arrived(ends.at[pl.ds(0, groups - 1)], send_ends)

    @pl.when(jnp.logical_or(gx == 0, gx == groups - 1))
    def _():
        arrived(side_parts, send_side)

    arrived(bests, recv_max)
    arrived(bests, send_max)
    peak = jnp.max(landed_ends[:, 1, :], axis=0, keepdims=True)
    for d in range(groups * (columns - 1)):
        peak = jnp.maximum(peak, bests[d])
    peak_out[...] = peak


def surface_by_kernel(coefficients, spacing, groups, columns):
    _, modes, ys = coefficients.shape
    full, twiddle = transform_tables()
    high = full.astype(jnp.bfloat16)
    low = (full - high.astype(np.float32)).astype(jnp.bfloat16)
    basis = np.concatenate([high, low], axis=0)
    weights = level_weights(spacing.shape[0])
    levels = spacing.shape[0] + 1
    count = NX // groups
    own = count // RADIX
    width = RADIX * TILE
    vmem = pl.BlockSpec(memory_space=pltpu.VMEM)
    hbm = pl.BlockSpec(memory_space=pltpu.HBM)
    dma = pltpu.SemaphoreType.DMA
    f32 = jnp.float32
    return pl.pallas_call(
        functools.partial(surface_kernel, groups, columns),
        out_shape=(
            pltpu.VMEM((count + 2 * TILE, ys), f32),
            pltpu.VMEM((2, TILE, LANES), f32),
            pltpu.VMEM((4, levels, LANES), f32),
            pltpu.VMEM((1, LANES), f32),
        ),
        in_specs=[hbm] * 5,
        out_specs=(vmem,) * 4,
        scratch_shapes=[
            pltpu.VMEM(coefficients.shape, f32),
            pltpu.VMEM((1, spacing.shape[0]), f32),
            pltpu.VMEM(weights.shape, f32),
            pltpu.VMEM(basis.shape, jnp.bfloat16),
            pltpu.VMEM(twiddle.shape, f32),
            pltpu.VMEM((ys, 2 * modes), f32),
            pltpu.VMEM((2, groups, TILE, 2 * modes), f32),
            pltpu.VMEM((2 * width, 2 * modes), jnp.bfloat16),
        ]
        + [pltpu.VMEM((groups, own, LANES), f32)] * 4
        + [
            pltpu.VMEM((groups, 2, LANES), f32),
            pltpu.VMEM((groups, 2, LANES), f32),
            pltpu.VMEM((groups, TILE, LANES), f32),
            pltpu.VMEM((2, TILE, LANES), f32),
            pltpu.VMEM((1, LANES), f32),
            pltpu.VMEM((groups * (columns - 1), 1, LANES), f32),
            pltpu.VMEM((groups, own, LANES), f32),
            dma((5,)),
            dma(()),
            dma((2,)),
            dma(()),
            dma((2,)),
            dma(()),
            dma(()),
            dma(()),
            dma((2,)),
            dma(()),
            dma(()),
            pltpu.SemaphoreType.REGULAR,
        ],
        compiler_params=pltpu.CompilerParams(
            collective_id=0, has_side_effects=True, vmem_limit_bytes=12 << 20
        ),
    )(*[
        pltpu.with_memory_space_constraint(jnp.asarray(x), pltpu.HBM)
        for x in (coefficients, spacing[None], weights, basis, twiddle)
    ])


def surface_by_gather(coefficients, spacing, groups):
    x_count = NX // groups
    x_first = lax.axis_index("gx") * x_count
    x_cells = x_first + jnp.arange(x_count, dtype=jnp.int32)
    portion = lax.all_gather(coefficients, "gx", axis=1, tiled=True)
    cosine, sine = basis(portion.shape[1], x_cells)
    surface = TOPO_SCALE * jnp.tanh(project(cosine, sine, portion) * 0.25)
    stretch = stretching(spacing)
    scale = stretch.shape[0] - 1.0
    slope = vertical(stretch)
    peak = lax.pmax(jnp.max(surface), ("gx", "gy"))
    wide = extended(surface, (("gx", 0), ("gy", 1)), 2)
    dx = (8.0 * (wide[3:-1] - wide[1:-3]) - (wide[4:] - wide[:-4]))[:, 2:-2] / 12.0
    dy = (8.0 * (wide[:, 3:-1] - wide[:, 1:-3]) - (wide[:, 4:] - wide[:, :-4]))[2:-2] / 12.0
    rows = [scale * stretch, scale * (1.0 - stretch), scale * slope]
    rows.append(slope / ((1.0 - peak) * jnp.min(slope)))
    table = jnp.broadcast_to(jnp.stack(rows)[:, :, None], (4, stretch.shape[0], LANES))
    return surface, dx, dy, table


def levels_kernel(depth, s_ref, dx_ref, dy_ref, table, z_ref, slopes_ref, jac_ref, quality_ref):
    first = pl.program_id(0) * depth

    def row(which, level):
        return table[which, pl.ds(first + level, 1), :]

    for level in range(depth):
        s, gain = s_ref[...], row(1, level)
        z_ref[level] = row(0, level) + gain * s
        slopes_ref[0, level] = gain * dx_ref[...]
        slopes_ref[1, level] = gain * dy_ref[...]
        rest = 1.0 - s
        jac_ref[level] = row(2, level) * rest
        quality_ref[level] = row(3, level) * rest


def all_levels(s, dx, dy, table):
    levels = table.shape[1]
    rows, columns = s.shape
    depth = 2
    plane = pl.BlockSpec((rows, columns), lambda i: (0, 0))
    field = pl.BlockSpec((depth, rows, columns), lambda i: (i, 0, 0))
    shape = jax.ShapeDtypeStruct((levels, rows, columns), jnp.float32)
    return pl.pallas_call(
        functools.partial(levels_kernel, depth),
        grid=(levels // depth,),
        in_specs=[plane, plane, plane, pl.BlockSpec(table.shape, lambda i: (0, 0, 0))],
        out_specs=(
            field,
            pl.BlockSpec((2, depth, rows, columns), lambda i: (0, i, 0, 0)),
            field,
            field,
        ),
        out_shape=(
            shape,
            jax.ShapeDtypeStruct((2, levels, rows, columns), jnp.float32),
            shape,
            shape,
        ),
    )(s, dx, dy, table)


def write_kernel(
    s_ref, sides, table, peak, z_hbm, slopes_hbm, jac_hbm, quality_hbm,
    z, slopes, jac, quality, dx, dy, outer, scaled, sems,
):
    levels, count, _ = z.shape
    own = count // RADIX
    inner = pl.ds(TILE, count)

    def row(which, level):
        return table[which, pl.ds(level, 1), :]

    def put(src, dst, at, which):
        pltpu.make_async_copy(src.at[at], dst.at[at], sems.at[which]).start()

    def heights(level, carry):
        s = s_ref[inner, :]
        z[level] = row(0, level) + row(1, level) * s
        put(z, z_hbm, level, 0)
        jac[level] = row(2, level) * (1.0 - s)
        put(jac, jac_hbm, level, 2)
        return carry

    lax.fori_loop(0, levels, heights, 0)
    highest = surface(jnp.max(peak[...], axis=1, keepdims=True))
    scaled[...] = table[3] / (1.0 - highest)

    def near(by):
        return s_ref[pl.ds(TILE + by, count), :]

    dx[...] = (8.0 * (near(1) - near(-1)) - (near(2) - near(-2))) * (1.0 / 12.0)
    lane = lax.broadcasted_iota(jnp.int32, (TILE, LANES), 1)
    for r in range(RADIX):
        for k in range(own // TILE):
            shift = LANES - r * TILE - 2 * k
            right = pltpu.roll(sides[0], shift % LANES, 1) if shift % LANES else sides[0]
            left = pltpu.roll(sides[1], (shift - 2) % LANES, 1) if (shift - 2) % LANES else sides[1]
            outer[pl.ds(k * TILE * RADIX + r, TILE, stride=RADIX), :] = jnp.where(
                lane < LANES // 2, right, left
            )
    s, edge = s_ref[inner, :], outer[...]
    lane = lax.broadcasted_iota(jnp.int32, (count, LANES), 1)

    def moved(by):
        taken = lane < by if by > 0 else lane >= LANES + by
        return pltpu.roll(jnp.where(taken, edge, s), (LANES - by) % LANES, 1)

    dy[...] = (8.0 * (moved(1) - moved(-1)) - (moved(2) - moved(-2))) * (1.0 / 12.0)

    def tilts(level, carry):
        gain = row(1, level)
        for at, slope in enumerate((dx, dy)):
            slopes[at, level] = gain * slope[...]
            put(slopes, slopes_hbm, (at, level), 1)
        quality[level] = scaled[pl.ds(level, 1), :] * (1.0 - s_ref[inner, :])
        put(quality, quality_hbm, level, 3)
        return carry

    lax.fori_loop(0, levels, tilts, 0)
    for i, (src, dst) in enumerate(
        ((z, z_hbm), (slopes, slopes_hbm), (jac, jac_hbm), (quality, quality_hbm))
    ):
        pltpu.make_async_copy(src, dst, sems.at[i]).wait()


def write_all(s, sides, table, peak):
    levels = table.shape[1]
    count, columns = s.shape[0] - 2 * TILE, s.shape[1]
    vmem = pl.BlockSpec(memory_space=pltpu.VMEM)
    hbm = pl.BlockSpec(memory_space=pl.ANY)
    field = (levels, count, columns)
    fields = (field, (2,) + field, field, field)
    f32 = jnp.float32
    plane = pltpu.VMEM((count, columns), f32)
    return pl.pallas_call(
        write_kernel,
        in_specs=[vmem] * 4,
        out_specs=(hbm,) * 4,
        out_shape=tuple(jax.ShapeDtypeStruct(shape, f32) for shape in fields),
        scratch_shapes=[pltpu.VMEM(shape, f32) for shape in fields]
        + [plane, plane, plane, pltpu.VMEM((levels, LANES), f32), pltpu.SemaphoreType.DMA((4,))],
        compiler_params=pltpu.CompilerParams(vmem_limit_bytes=48 << 20),
    )(s, sides, table, peak)


def shards(coefficients, spacing):
    groups, columns = lax.axis_size("gx"), lax.axis_size("gy")
    _, modes, ys = coefficients.shape
    fits = (
        groups == 8
        and ys == LANES
        and ys == groups * RADIX
        and modes == NX // RADIX
        and modes % LANES == 0
        and columns > 1
    )
    if fits:
        return write_all(*surface_by_kernel(coefficients, spacing, groups, columns))
    return all_levels(*surface_by_gather(coefficients, spacing, groups))


def solution(mesh):
    return jax.shard_map(
        shards,
        mesh=mesh,
        in_specs=(P(None, "gx", "gy"), P()),
        out_specs=(
            P(None, "gx", "gy"),
            P(None, None, "gx", "gy"),
            P(None, "gx", "gy"),
            P(None, "gx", "gy"),
        ),
        check_vma=False,
    )
```

```python
import functools
import math

import jax
import jax.numpy as jnp
import numpy as np
from jax import lax
from jax.experimental import pallas as pl
from jax.experimental.pallas import tpu as pltpu
from jax.sharding import PartitionSpec as P

NX = 4096


BOUNDARY = (
    (-24.0 / 17.0, 59.0 / 34.0, -4.0 / 17.0, -3.0 / 34.0, 0.0, 0.0),
    (-0.5, 0.0, 0.5, 0.0, 0.0, 0.0),
    (4.0 / 43.0, -59.0 / 86.0, 0.0, 59.0 / 86.0, -4.0 / 43.0, 0.0),
    (3.0 / 98.0, 0.0, -59.0 / 98.0, 0.0, 32.0 / 49.0, -4.0 / 49.0),
)
TOPO_SCALE = 0.1


def extended(cells, sides, width):
    for axis, dim in sides:
        count = lax.axis_size(axis)
        head = lax.slice_in_dim(cells, 0, width, axis=dim)
        tail = lax.slice_in_dim(cells, cells.shape[dim] - width, cells.shape[dim], axis=dim)
        cells = jnp.concatenate(
            [
                lax.ppermute(tail, axis, [(i, (i + 1) % count) for i in range(count)]),
                cells,
                lax.ppermute(head, axis, [((i + 1) % count, i) for i in range(count)]),
            ],
            axis=dim,
        )
    return cells


def vertical(field):
    levels = field.shape[0]
    top_rows = []
    bottom_rows = []
    for row_id in range(4):
        upper = None
        lower = None
        for level_id, factor in enumerate(BOUNDARY[row_id]):
            if factor != 0.0:
                term_up = factor * field[level_id]
                term_down = -factor * field[levels - 1 - level_id]
                upper = term_up if upper is None else upper + term_up
                lower = term_down if lower is None else lower + term_down
        top_rows.append(upper)
        bottom_rows.append(lower)
    inner = (
        8.0 * (field[5 : levels - 3] - field[3 : levels - 5])
        - (field[6 : levels - 2] - field[2 : levels - 6])
    ) / 12.0
    return jnp.concatenate([jnp.stack(top_rows), inner, jnp.stack(bottom_rows[::-1])], axis=0)


def stretching(spacing):
    summed = jnp.sum(spacing)
    return jnp.concatenate([jnp.zeros((1,), spacing.dtype), jnp.cumsum(spacing)]) / summed


def column_depth(surface, stretch):
    levels = stretch.shape[0]
    return (levels - 1.0) * (surface[None] + (1.0 - surface[None]) * stretch[:, None, None])


def basis(count, x_cells):
    mode_ids = jnp.arange(count, dtype=jnp.int32)
    phase = (mode_ids[:, None] * x_cells[None, :] % NX).astype(jnp.float32) * (2.0 * math.pi / NX)
    return (jnp.cos(phase), jnp.sin(phase))


def project(cosine, sine, portion):
    first = jnp.dot(
        cosine.T, portion[0], precision=lax.Precision.HIGHEST, preferred_element_type=jnp.float32
    )
    return first + jnp.dot(
        sine.T, portion[1], precision=lax.Precision.HIGHEST, preferred_element_type=jnp.float32
    )


LANES = 128
RADIX = 16
TILE = 8
MESH = pl.DeviceIdType.MESH


def level_weights(gaps):
    levels = gaps + 1
    summed = np.tril(np.ones((levels, gaps)), -1)
    deriv = np.zeros((levels, levels))
    for row in range(levels):
        if row < 4:
            deriv[row, :6] = BOUNDARY[row]
        elif row >= levels - 4:
            deriv[row, ::-1][:6] = -np.array(BOUNDARY[levels - 1 - row])
        else:
            deriv[row, row - 2 : row + 3] = np.array([1.0, -8.0, 0.0, 8.0, -1.0]) / 12.0
    return np.stack([summed, deriv @ summed]).astype(np.float32)


def transform_tables():
    part = NX // RADIX
    angle = 2.0 * np.pi / part * ((np.arange(part)[:, None] * np.arange(part)[None]) % part)
    full = np.concatenate([np.cos(angle), np.sin(angle)], axis=1).astype(np.float32)
    turn = 2.0 * np.pi / NX * (np.arange(RADIX)[:, None] * np.arange(part)[None])
    twiddle = np.concatenate([np.cos(turn), np.sin(turn)], axis=1).astype(np.float32)
    return full, twiddle


def rotate(value, angle):
    re, im = value
    cos, sin = math.cos(angle), math.sin(angle)
    if abs(sin) < 1e-12:
        return (re, im) if cos > 0 else (-re, -im)
    if abs(cos) < 1e-12:
        return (im, -re) if sin > 0 else (-im, re)
    if abs(abs(cos) - abs(sin)) < 1e-12:
        unit = math.sqrt(0.5)
        a, b = math.copysign(1.0, cos), math.copysign(1.0, sin)
        one = re * unit if a > 0 else re * -unit
        two = im * unit if a > 0 else im * -unit
        if a == b:
            return one + two, two - one
        return one - two, two + one
    return re * cos + im * sin, im * cos - re * sin


def fourier(values):
    count = len(values)
    if count == 1:
        return values
    even, odd = fourier(values[0::2]), fourier(values[1::2])
    out = [None] * count
    for i in range(count // 2):
        re, im = rotate(odd[i], 2.0 * math.pi * i / count)
        out[i] = (even[i][0] + re, even[i][1] + im)
        out[i + count // 2] = (even[i][0] - re, even[i][1] - im)
    return out


def split(value):
    high = value.astype(jnp.bfloat16)
    return high, (value - high.astype(jnp.float32)).astype(jnp.bfloat16)


def butterfly(values, bit, lane):
    shift = bit * TILE
    upper = (lane // TILE) & bit != 0
    for i in sorted(values):
        if not i & bit and i | bit in values:
            low, high = values[i], values[i | bit]
            values[i] = jnp.where(upper, pltpu.roll(high, shift, 1), low)
            values[i | bit] = jnp.where(upper, high, pltpu.roll(low, LANES - shift, 1))
    return values


def blocks_of(chunk, groups):
    return [2 * j + (chunk + j // (groups // 2)) % 2 for j in range(groups)]


def surface(raw):
    return TOPO_SCALE * jnp.tanh(raw * 0.25)


def arrived(view, sem):
    pltpu.make_async_copy(view, view, sem).wait()


def surface_kernel(
    groups, columns, coef_hbm, spacing_hbm, weights_hbm, basis_hbm, twiddle_hbm,
    s_out, sides, table, peak_out,
    coef, spacing, weights, basis, twiddle, turned, gathered, operand,
    product_one, product_two, landed_one, landed_two, ends, landed_ends,
    side_parts, landed_sides, best, bests, partial,
    load_sem, send_one, recv_one, send_two, recv_two, send_ends, recv_ends,
    send_side, recv_side, send_max, recv_max, later_sem,
):
    gx, gy = lax.axis_index("gx"), lax.axis_index("gy")
    cores, rows_of = 2, groups // 2
    flip = gx // rows_of
    col, core = gx // cores - flip * (rows_of // cores), gx - gx // cores * cores

    def other(d):
        places = (flip, d // rows_of), (col, d // cores % 2), (core, d % cores)
        row_to, col_to, core_to = [1 - at if moves else at for at, moves in places]
        return row_to * rows_of + col_to * cores + core_to

    peers = [other(d) for d in (6, 7, 2, 3, 4, 5, 1)]
    loads = [
        pltpu.make_async_copy(src, dst, load_sem.at[i])
        for i, (src, dst) in enumerate((
            (coef_hbm, coef),
            (spacing_hbm, spacing),
            (weights_hbm, weights),
            (twiddle_hbm, twiddle),
            (basis_hbm, basis),
        ))
    ]
    loads[0].start()
    barrier = pltpu.get_barrier_semaphore()
    for peer in peers:
        pl.semaphore_signal(barrier, inc=1, device_id=(peer, gy), device_id_type=MESH)
    for up in range(1, columns):

        @pl.when(gy + up < columns)
        def _():
            for d in range(groups):
                target = (lax.rem(gx + d, groups), gy + up)
                pl.semaphore_signal(barrier, inc=1, device_id=target, device_id_type=MESH)

    part = coef.shape[1]
    ys = coef.shape[2] // groups
    half = NX // RADIX

    def sub_of(chunk, target):
        return lax.rem(chunk + target // rows_of, 2)

    def turned_rows(chunk, target):
        return pl.ds(pl.multiple_of(target * ys + sub_of(chunk, target) * TILE, TILE), TILE)

    loads[0].wait()
    for load in loads[1:]:
        load.start()
    turned[:, :part] = coef[0].T
    turned[:, part:] = coef[1].T
    pl.semaphore_wait(barrier, groups - 1 + groups * gy)

    far, close = peers[:2], peers[2:]
    order = [(chunk, peer) for some in (far, close) for chunk in range(2) for peer in some]
    for chunk, target in order:
        pltpu.make_async_remote_copy(
            src_ref=turned.at[turned_rows(chunk, target)],
            dst_ref=gathered.at[chunk, gx],
            send_sem=send_one,
            recv_sem=recv_one.at[chunk],
            device_id=(target, gy),
            device_id_type=MESH,
        ).start()
    for down in range(1, columns):

        @pl.when(gy >= down)
        def _():
            for d in range(groups):
                target = (lax.rem(gx + d, groups), gy - down)
                pl.semaphore_signal(later_sem, inc=1, device_id=target, device_id_type=MESH)

    for chunk in range(2):
        gathered[chunk, gx] = turned[turned_rows(chunk, gx), :]

    for load in loads[1:]:
        load.wait()
    thick = spacing[...]
    total = jnp.sum(thick, axis=1, keepdims=True)
    scale = spacing.shape[1] * 1.0
    levels = spacing.shape[1] + 1
    stretch = jnp.sum(weights[0] * thick, axis=1, keepdims=True) / total
    slope = jnp.sum(weights[1] * thick, axis=1, keepdims=True) / total
    least = jnp.min(slope, axis=0, keepdims=True)
    table[0] = jnp.broadcast_to(scale * stretch, (levels, LANES))
    table[1] = jnp.broadcast_to(scale * (1.0 - stretch), (levels, LANES))
    table[2] = jnp.broadcast_to(scale * slope, (levels, LANES))
    table[3] = jnp.broadcast_to(slope / least, (levels, LANES))

    rows = basis.shape[0] // 2
    own = rows // groups
    count = own * RADIX
    width = RADIX * TILE
    dot = functools.partial(
        lax.dot_general,
        dimension_numbers=(((1,), (1,)), ((), ())),
        preferred_element_type=jnp.float32,
    )

    def transform(chunk):
        values = [
            (gathered[chunk, i, :, :part], gathered[chunk, i, :, part:]) for i in range(groups)
        ]
        even = fourier(values)
        odd = fourier([rotate(v, 2.0 * math.pi * i / RADIX) for i, v in enumerate(values)])
        for r in range(0, RADIX, 2):
            pair = []
            for k, (re, im) in ((r, even[r // 2]), (r + 1, odd[r // 2])):
                if k:
                    cos, sin = twiddle[k : k + 1, :half], twiddle[k : k + 1, half:]
                    re, im = re * cos + im * sin, im * cos - re * sin
                pair.append((re, im))
            for at, lanes in enumerate((slice(0, half), slice(half, 2 * half))):
                high, low = split(jnp.concatenate([pair[0][at], pair[1][at]], axis=0))
                operand[r * TILE : (r + 2) * TILE, lanes] = high
                operand[width + r * TILE : width + (r + 2) * TILE, lanes] = low
        small = dot(basis[rows:], operand[:width])
        both = dot(basis[:rows], operand[...])
        return both[:, :width] + (both[:, width:] + small)

    def send_product(chunk, some):
        product, landed = ((product_one, landed_one), (product_two, landed_two))[chunk]
        for target in some:
            pltpu.make_async_remote_copy(
                src_ref=product.at[target],
                dst_ref=landed.at[gx],
                send_sem=send_two,
                recv_sem=recv_two.at[chunk],
                device_id=(target, gy),
                device_id_type=MESH,
            ).start()

    def tallest(raw):
        return functools.reduce(jnp.maximum, [raw[i : i + TILE] for i in range(0, rows, TILE)])

    row_lane = lax.broadcasted_iota(jnp.int32, (1, LANES), 1)

    def ends_of(raw):
        return [
            jnp.where(
                row_lane < LANES // 2,
                raw[(dest + 1) * own % rows : (dest + 1) * own % rows + 1],
                raw[(dest * own - 1) % rows : (dest * own - 1) % rows + 1],
            )
            for dest in range(groups)
        ]

    def send_best(target, slot):
        for d in range(groups):
            pltpu.make_async_remote_copy(
                src_ref=best,
                dst_ref=bests.at[slot * groups + gx],
                send_sem=send_max,
                recv_sem=recv_max,
                device_id=(lax.rem(gx + d, groups), target),
                device_id_type=MESH,
            ).start()

    lane_one = lax.broadcasted_iota(jnp.int32, (TILE, LANES), 1)

    def pack_sides():
        for dest in range(groups):
            packed = None
            for k in range(own // TILE):
                shift = jnp.where(flip == 0, 2 * k, (2 * k + 2 - TILE) % LANES)
                tile = pltpu.roll(product_one[dest, k * TILE : (k + 1) * TILE], shift, 1)
                packed = tile if k == 0 else jnp.where(lane_one % TILE // 2 == k, tile, packed)
            side_parts[dest] = packed

    def send_sides(to_lower):
        for which, sender in enumerate((0, groups - 1)):
            column = lax.rem(gy + (columns - 1, 1)[which], columns)

            @pl.when(jnp.logical_and(gx == sender, (column < gy) if to_lower else (column > gy)))
            def _():
                for dest in range(groups):
                    pltpu.make_async_remote_copy(
                        src_ref=side_parts.at[dest],
                        dst_ref=landed_sides.at[which],
                        send_sem=send_side,
                        recv_sem=recv_side.at[which],
                        device_id=(dest, column),
                        device_id_type=MESH,
                    ).start()

    arrived(gathered.at[0, pl.ds(0, groups - 1)], recv_one.at[0])
    raw = transform(0)
    for dest in range(groups):
        product_one[dest] = raw[dest * own : (dest + 1) * own]
    by_col, by_row, twin = close[:2], close[2:4], close[4:]
    send_product(0, far + by_col + twin)
    landed_one[gx] = product_one[gx]
    ends_one = ends_of(raw)
    peak_one = tallest(raw)

    arrived(gathered.at[1, pl.ds(0, groups - 1)], recv_one.at[1])
    raw = transform(1)
    for dest in range(groups):
        product_two[dest] = raw[dest * own : (dest + 1) * own]
    best[...] = jnp.max(jnp.maximum(peak_one, tallest(raw)), axis=0, keepdims=True)
    for down in range(columns - 1, 0, -1):

        @pl.when(gy >= down)
        def _():
            send_best(gy - down, down - 1)

        if down == columns - 1:
            pack_sides()
            send_sides(True)

    send_product(1, far)
    send_product(0, by_row)
    send_product(1, by_col + twin + by_row)
    landed_two[gx] = product_two[gx]
    ends_two = ends_of(raw)
    outside = jnp.abs(row_lane // TILE * 2 - (RADIX - 1)) > RADIX // 2
    for dest in range(groups):
        one, two = ends_one[dest], ends_two[dest]
        low, high = jnp.where(flip == 0, one, two), jnp.where(flip == 0, two, one)
        ends[dest, 0:1] = jnp.where(outside, low, pltpu.roll(high, LANES // 2, 1))
        ends[dest, 1:2] = best[...]
    for target in peers:
        pltpu.make_async_remote_copy(
            src_ref=ends.at[target],
            dst_ref=landed_ends.at[gx],
            send_sem=send_ends,
            recv_sem=recv_ends,
            device_id=(target, gy),
            device_id_type=MESH,
        ).start()
    landed_ends[gx] = ends[gx]

    @pl.when(gy < columns - 1)
    def _():
        pl.semaphore_wait(later_sem, groups * (columns - 1 - gy))

    send_sides(False)

    for up in range(1, columns):

        @pl.when(gy + up < columns)
        def _():
            send_best(gy + up, columns - up - 1)

    lane = lax.broadcasted_iota(jnp.int32, (own, LANES), 1)
    arrived(landed_one.at[pl.ds(0, groups - 1)], recv_two.at[0])
    first = {b: surface(landed_one[j]) for j, b in enumerate(blocks_of(0, groups))}
    for bit in (2, 4):
        first = butterfly(first, bit, lane)
    for b, value in first.items():
        partial[b // 2] = value

    arrived(landed_two.at[pl.ds(0, groups - 1)], recv_two.at[1])
    second = {b: surface(landed_two[j]) for j, b in enumerate(blocks_of(1, groups))}
    for bit in (2, 4):
        second = butterfly(second, bit, lane)
    pieces = {b: partial[b // 2] for b in first} | second
    for bit in (8, 1):
        pieces = butterfly(pieces, bit, lane)
    for r in range(RADIX):
        s_out[pl.ds(TILE + r, own, stride=RADIX), :] = pieces[r]

    arrived(landed_ends.at[pl.ds(0, groups - 1)], recv_ends)
    edge = pltpu.roll(surface(landed_ends[:, 0, :]), 0, 1, stride=2 * TILE, stride_axis=0)
    lane = lax.broadcasted_iota(jnp.int32, (groups, LANES), 1)
    source = lax.broadcasted_iota(jnp.int32, (groups, LANES), 0)
    for at, r in ((-2, RADIX - 2), (-1, RADIX - 1), (count, 0), (count + 1, 1)):
        total_row = None
        for sub in range(2):
            shift = (sub - (r - sub * RADIX // 2)) * TILE % LANES
            moved = pltpu.roll(edge, shift, 1) if shift else edge
            moved = jnp.where(lane // TILE == 2 * source + sub, moved, 0.0)
            total_row = moved if sub == 0 else total_row + moved
        s_out[TILE + at : TILE + at + 1, :] = jnp.sum(total_row, axis=0, keepdims=True)

    for which in range(2):
        arrived(landed_sides.at[which], recv_side.at[which])
        sides[which] = surface(landed_sides[which])

    arrived(turned.at[pl.ds(0, (groups - 1) * ys)], send_one)
    arrived(product_one.at[pl.ds(0, groups - 1)], send_two)
    arrived(product_two.at[pl.ds(0, groups - 1)], send_two)
    arrived(ends.at[pl.ds(0, groups - 1)], send_ends)

    @pl.when(jnp.logical_or(gx == 0, gx == groups - 1))
    def _():
        arrived(side_parts, send_side)

    arrived(bests, recv_max)
    arrived(bests, send_max)
    peak = jnp.max(landed_ends[:, 1, :], axis=0, keepdims=True)
    for d in range(groups * (columns - 1)):
        peak = jnp.maximum(peak, bests[d])
    peak_out[...] = peak


def surface_by_kernel(coefficients, spacing, groups, columns):
    _, modes, ys = coefficients.shape
    full, twiddle = transform_tables()
    high = full.astype(jnp.bfloat16)
    low = (full - high.astype(np.float32)).astype(jnp.bfloat16)
    basis = np.concatenate([high, low], axis=0)
    weights = level_weights(spacing.shape[0])
    levels = spacing.shape[0] + 1
    count = NX // groups
    own = count // RADIX
    width = RADIX * TILE
    vmem = pl.BlockSpec(memory_space=pltpu.VMEM)
    hbm = pl.BlockSpec(memory_space=pltpu.HBM)
    dma = pltpu.SemaphoreType.DMA
    f32 = jnp.float32
    return pl.pallas_call(
        functools.partial(surface_kernel, groups, columns),
        out_shape=(
            pltpu.VMEM((count + 2 * TILE, ys), f32),
            pltpu.VMEM((2, TILE, LANES), f32),
            pltpu.VMEM((4, levels, LANES), f32),
            pltpu.VMEM((1, LANES), f32),
        ),
        in_specs=[hbm] * 5,
        out_specs=(vmem,) * 4,
        scratch_shapes=[
            pltpu.VMEM(coefficients.shape, f32),
            pltpu.VMEM((1, spacing.shape[0]), f32),
            pltpu.VMEM(weights.shape, f32),
            pltpu.VMEM(basis.shape, jnp.bfloat16),
            pltpu.VMEM(twiddle.shape, f32),
            pltpu.VMEM((ys, 2 * modes), f32),
            pltpu.VMEM((2, groups, TILE, 2 * modes), f32),
            pltpu.VMEM((2 * width, 2 * modes), jnp.bfloat16),
        ]
        + [pltpu.VMEM((groups, own, LANES), f32)] * 4
        + [
            pltpu.VMEM((groups, 2, LANES), f32),
            pltpu.VMEM((groups, 2, LANES), f32),
            pltpu.VMEM((groups, TILE, LANES), f32),
            pltpu.VMEM((2, TILE, LANES), f32),
            pltpu.VMEM((1, LANES), f32),
            pltpu.VMEM((groups * (columns - 1), 1, LANES), f32),
            pltpu.VMEM((groups, own, LANES), f32),
            dma((5,)),
            dma(()),
            dma((2,)),
            dma(()),
            dma((2,)),
            dma(()),
            dma(()),
            dma(()),
            dma((2,)),
            dma(()),
            dma(()),
            pltpu.SemaphoreType.REGULAR,
        ],
        compiler_params=pltpu.CompilerParams(
            collective_id=0, has_side_effects=True, vmem_limit_bytes=12 << 20
        ),
    )(*[
        pltpu.with_memory_space_constraint(jnp.asarray(x), pltpu.HBM)
        for x in (coefficients, spacing[None], weights, basis, twiddle)
    ])


def surface_by_gather(coefficients, spacing, groups):
    x_count = NX // groups
    x_first = lax.axis_index("gx") * x_count
    x_cells = x_first + jnp.arange(x_count, dtype=jnp.int32)
    portion = lax.all_gather(coefficients, "gx", axis=1, tiled=True)
    cosine, sine = basis(portion.shape[1], x_cells)
    surface = TOPO_SCALE * jnp.tanh(project(cosine, sine, portion) * 0.25)
    stretch = stretching(spacing)
    scale = stretch.shape[0] - 1.0
    slope = vertical(stretch)
    peak = lax.pmax(jnp.max(surface), ("gx", "gy"))
    wide = extended(surface, (("gx", 0), ("gy", 1)), 2)
    dx = (8.0 * (wide[3:-1] - wide[1:-3]) - (wide[4:] - wide[:-4]))[:, 2:-2] / 12.0
    dy = (8.0 * (wide[:, 3:-1] - wide[:, 1:-3]) - (wide[:, 4:] - wide[:, :-4]))[2:-2] / 12.0
    rows = [scale * stretch, scale * (1.0 - stretch), scale * slope]
    rows.append(slope / ((1.0 - peak) * jnp.min(slope)))
    table = jnp.broadcast_to(jnp.stack(rows)[:, :, None], (4, stretch.shape[0], LANES))
    return surface, dx, dy, table


def levels_kernel(depth, s_ref, dx_ref, dy_ref, table, z_ref, slopes_ref, jac_ref, quality_ref):
    first = pl.program_id(0) * depth

    def row(which, level):
        return table[which, pl.ds(first + level, 1), :]

    for level in range(depth):
        s, gain = s_ref[...], row(1, level)
        z_ref[level] = row(0, level) + gain * s
        slopes_ref[0, level] = gain * dx_ref[...]
        slopes_ref[1, level] = gain * dy_ref[...]
        rest = 1.0 - s
        jac_ref[level] = row(2, level) * rest
        quality_ref[level] = row(3, level) * rest


def all_levels(s, dx, dy, table):
    levels = table.shape[1]
    rows, columns = s.shape
    depth = 2
    plane = pl.BlockSpec((rows, columns), lambda i: (0, 0))
    field = pl.BlockSpec((depth, rows, columns), lambda i: (i, 0, 0))
    shape = jax.ShapeDtypeStruct((levels, rows, columns), jnp.float32)
    return pl.pallas_call(
        functools.partial(levels_kernel, depth),
        grid=(levels // depth,),
        in_specs=[plane, plane, plane, pl.BlockSpec(table.shape, lambda i: (0, 0, 0))],
        out_specs=(
            field,
            pl.BlockSpec((2, depth, rows, columns), lambda i: (0, i, 0, 0)),
            field,
            field,
        ),
        out_shape=(
            shape,
            jax.ShapeDtypeStruct((2, levels, rows, columns), jnp.float32),
            shape,
            shape,
        ),
    )(s, dx, dy, table)


def write_kernel(
    s_ref, sides, table, peak, z_hbm, slopes_hbm, jac_hbm, quality_hbm,
    z, slopes, jac, quality, dx, dy, outer, scaled, sems,
):
    levels, count, _ = z.shape
    own = count // RADIX
    inner = pl.ds(TILE, count)

    def row(which, level):
        return table[which, pl.ds(level, 1), :]

    def put(src, dst, at, which):
        pltpu.make_async_copy(src.at[at], dst.at[at], sems.at[which]).start()

    def heights(level, carry):
        s = s_ref[inner, :]
        z[level] = row(0, level) + row(1, level) * s
        put(z, z_hbm, level, 0)
        jac[level] = row(2, level) * (1.0 - s)
        put(jac, jac_hbm, level, 2)
        return carry

    lax.fori_loop(0, levels, heights, 0)
    highest = surface(jnp.max(peak[...], axis=1, keepdims=True))
    scaled[...] = table[3] / (1.0 - highest)

    def near(by):
        return s_ref[pl.ds(TILE + by, count), :]

    dx[...] = (8.0 * (near(1) - near(-1)) - (near(2) - near(-2))) * (1.0 / 12.0)
    lane = lax.broadcasted_iota(jnp.int32, (TILE, LANES), 1)
    for r in range(RADIX):
        for k in range(own // TILE):
            shift = LANES - r * TILE - 2 * k
            right = pltpu.roll(sides[0], shift % LANES, 1) if shift % LANES else sides[0]
            left = pltpu.roll(sides[1], (shift - 2) % LANES, 1) if (shift - 2) % LANES else sides[1]
            outer[pl.ds(k * TILE * RADIX + r, TILE, stride=RADIX), :] = jnp.where(
                lane < LANES // 2, right, left
            )
    s, edge = s_ref[inner, :], outer[...]
    lane = lax.broadcasted_iota(jnp.int32, (count, LANES), 1)

    def moved(by):
        taken = lane < by if by > 0 else lane >= LANES + by
        return pltpu.roll(jnp.where(taken, edge, s), (LANES - by) % LANES, 1)

    dy[...] = (8.0 * (moved(1) - moved(-1)) - (moved(2) - moved(-2))) * (1.0 / 12.0)

    def tilts(level, carry):
        gain = row(1, level)
        for at, slope in enumerate((dx, dy)):
            slopes[at, level] = gain * slope[...]
            put(slopes, slopes_hbm, (at, level), 1)
        quality[level] = scaled[pl.ds(level, 1), :] * (1.0 - s_ref[inner, :])
        put(quality, quality_hbm, level, 3)
        return carry

    lax.fori_loop(0, levels, tilts, 0)
    for i, (src, dst) in enumerate(
        ((z, z_hbm), (slopes, slopes_hbm), (jac, jac_hbm), (quality, quality_hbm))
    ):
        pltpu.make_async_copy(src, dst, sems.at[i]).wait()


def write_all(s, sides, table, peak):
    levels = table.shape[1]
    count, columns = s.shape[0] - 2 * TILE, s.shape[1]
    vmem = pl.BlockSpec(memory_space=pltpu.VMEM)
    hbm = pl.BlockSpec(memory_space=pl.ANY)
    field = (levels, count, columns)
    fields = (field, (2,) + field, field, field)
    f32 = jnp.float32
    plane = pltpu.VMEM((count, columns), f32)
    return pl.pallas_call(
        write_kernel,
        in_specs=[vmem] * 4,
        out_specs=(hbm,) * 4,
        out_shape=tuple(jax.ShapeDtypeStruct(shape, f32) for shape in fields),
        scratch_shapes=[pltpu.VMEM(shape, f32) for shape in fields]
        + [plane, plane, plane, pltpu.VMEM((levels, LANES), f32), pltpu.SemaphoreType.DMA((4,))],
        compiler_params=pltpu.CompilerParams(vmem_limit_bytes=48 << 20),
    )(s, sides, table, peak)


def shards(coefficients, spacing):
    groups, columns = lax.axis_size("gx"), lax.axis_size("gy")
    _, modes, ys = coefficients.shape
    fits = (
        groups == 8
        and ys == LANES
        and ys == groups * RADIX
        and modes == NX // RADIX
        and modes % LANES == 0
        and columns > 1
    )
    if fits:
        return write_all(*surface_by_kernel(coefficients, spacing, groups, columns))
    return all_levels(*surface_by_gather(coefficients, spacing, groups))


def solution(mesh):
    return jax.shard_map(
        shards,
        mesh=mesh,
        in_specs=(P(None, "gx", "gy"), P()),
        out_specs=(
            P(None, "gx", "gy"),
            P(None, None, "gx", "gy"),
            P(None, "gx", "gy"),
            P(None, "gx", "gy"),
        ),
        check_vma=False,
    )
```
